32 devices in a mesh: dp: 2 (over x), cols: 4 (over z), rows: 4 (over y, core).
Axes of the slice: x: 2, y: 2, z: 4, core: 2. Of those that a mesh axis runs over, the one named last changes fastest.
Arguments:
- h_init: bfloat16 [2, 512, 128, 64], P('dp', 'rows', 'cols'), parts along dimension 0
- c_init: float32 [2, 512, 128, 64], P('dp', 'rows', 'cols'), parts along dimension 0
- w_rec: bfloat16 [3, 3, 64, 256], replicated
- gate_bias: float32 [32, 256], replicated
Outputs:
- output 1: bfloat16 [32, 2, 512, 128, 64], P(None, 'dp', 'rows', 'cols'), parts along dimension 1
- output 2: float32 [2, 512, 128, 64], P('dp', 'rows', 'cols'), parts along dimension 0
There are 2 independent parts. The reference program is written for one: setup_inputs(seed, part) draws one part's arguments, and reference() takes and returns one part's arrays. A program takes and returns all parts, laid end to end along the dimension named above; an argument that names none is the same for every part.
All inputs are finite; a program needn't handle non-finite values.
Results may differ from the reference program's by a relative error of at most 0.00444045.
Values are sent between devices in bfloat16 or wider.
A program may use at most 1 GiB of HBM per device.

```python
import jax
import jax.numpy as jnp
from jax import lax

STEPS = 32
BATCH = 1
GRID_H = 512
GRID_W = 128
CHANNELS = 64


def setup_inputs(seed: int = 0, part: int = 0) -> dict:
    key_w, key_b = jax.random.split(jax.random.key(seed))
    part_key = jax.random.fold_in(jax.random.key(seed + 1), part)
    key_h, key_c = jax.random.split(part_key)
    fan_in = 9 * CHANNELS
    w_rec = (jax.random.normal(key_w, (3, 3, CHANNELS, 4 * CHANNELS), jnp.float32) * (1.5 * fan_in ** -0.5)).astype(jnp.bfloat16)
    gate_offset = jnp.repeat(jnp.array([0.0, 1.0, 0.0, 0.0], jnp.float32), CHANNELS)
    gate_bias = jax.random.normal(key_b, (STEPS, 4 * CHANNELS), jnp.float32) * 0.5 + gate_offset
    h_init = (jax.random.normal(key_h, (BATCH, GRID_H, GRID_W, CHANNELS), jnp.float32) * 0.6).astype(jnp.bfloat16)
    c_init = jax.random.normal(key_c, (BATCH, GRID_H, GRID_W, CHANNELS), jnp.float32)
    return {"h_init": h_init, "c_init": c_init, "w_rec": w_rec, "gate_bias": gate_bias}


def reference(h_init, c_init, w_rec, gate_bias):
    w_wide = w_rec.astype(jnp.float32)

    def one_step(carry_in, bias_row):
        h_prev, c_prev = carry_in
        gate_pre = lax.conv_general_dilated(h_prev.astype(jnp.float32), w_wide, (1, 1), "SAME", dimension_numbers=("NHWC", "HWIO", "NHWC")) + bias_row
        in_gate, forget_gate, out_gate, cand_gate = jnp.split(gate_pre, 4, axis=-1)
        c_next = jax.nn.sigmoid(forget_gate) * c_prev + jax.nn.sigmoid(in_gate) * jnp.tanh(cand_gate)
        h_next = (jax.nn.sigmoid(out_gate) * jnp.tanh(c_next)).astype(jnp.bfloat16)
        return (h_next, c_next), h_next

    final_state, h_seq = lax.scan(one_step, (h_init, c_init), gate_bias)
    return h_seq, final_state[1]
```

```python
import functools

import jax
import jax.numpy as jnp
from jax import lax
from jax.experimental import pallas as pl
from jax.experimental.pallas import tpu as pltpu
from jax.sharding import PartitionSpec as P

UP, DOWN, LEFT, RIGHT, UP_LEFT, UP_RIGHT, DOWN_LEFT, DOWN_RIGHT = range(8)
OFFSETS = ((-1, 0), (1, 0), (0, -1), (0, 1), (-1, -1), (-1, 1), (1, -1), (1, 1))
OPPOSITE = (DOWN, UP, RIGHT, LEFT, DOWN_RIGHT, DOWN_LEFT, UP_RIGHT, UP_LEFT)
EDGE_DIRS = (UP, DOWN, UP_LEFT, UP_RIGHT, DOWN_LEFT, DOWN_RIGHT)
MESH = pl.DeviceIdType.MESH


def kernel(steps, tiles, chunks, rows_n, cols_n, h_init, c_init, w_ref, bias_ref, h_seq, c_last,
           hl0, hr0, hl1, hr1, cs, bs, ghost, pack_e, pack_c, recv_e, recv_c,
           init_sem, out_sem, send_col, recv_col, send_e, recv_e_sem, send_c, recv_c_sem):
    ch, lanes = h_init.shape[1], h_init.shape[2]
    cols = 2 * tiles
    groups = ch // 16
    stacks = ((hl0, hr0), (hl1, hr1))
    row, col = lax.axis_index("rows"), lax.axis_index("cols")
    chunk_of = {j: (k, j - chunk[0]) for k, chunk in enumerate(chunks) for j in chunk}

    has, target, slot = [], [], []
    for d, (dr, dc) in enumerate(OFFSETS):
        r, c = row + dr, col + dc
        has.append((r >= 0) & (r < rows_n) & (c >= 0) & (c < cols_n))
        target.append({"rows": r, "cols": c})
        slot.append(OPPOSITE[d])

    def at(d, action):
        pl.when(has[d])(action)

    for ref in (ghost, recv_e, recv_c):
        ref[...] = jnp.zeros_like(ref)
    barrier = pltpu.get_barrier_semaphore()
    for d in range(8):
        at(d, lambda d=d: pl.semaphore_signal(barrier, inc=1, device_id=target[d], device_id_type=MESH))
    around_r = 1 + has[UP].astype(jnp.int32) + has[DOWN].astype(jnp.int32)
    around_c = 1 + has[LEFT].astype(jnp.int32) + has[RIGHT].astype(jnp.int32)
    pl.semaphore_wait(barrier, around_r * around_c - 1)

    def column(side, j):
        return j if side == 0 else cols - 1 - j

    loads = []
    for side in range(2):
        for j in range(tiles):
            loads.append(pltpu.make_async_copy(h_init.at[column(side, j)], stacks[0][side].at[j + 1, pl.ds(ch, ch)], init_sem.at[0, side, j]))
            loads.append(pltpu.make_async_copy(c_init.at[column(side, j)], cs.at[side, j], init_sem.at[1, side, j]))
    for copy in loads:
        copy.start()
    for copy in loads:
        copy.wait()

    lane = lax.broadcasted_iota(jnp.int16, (16, lanes), 1)
    pair_of = lax.shift_right_logical(lane, jnp.int16(1))
    even = (lane & jnp.int16(1)) == jnp.int16(0)
    first, last = lane == jnp.int16(0), lane == jnp.int16(lanes - 1)
    zero = jnp.zeros((16, lanes), jnp.bfloat16)

    def pack(packed, local, side, h):
        for g in range(groups):
            pair = 16 * g + 2 * local + side
            moved = pltpu.roll(h[16 * g:16 * g + 16], (1 + 2 * pair) % lanes, 1)
            packed = jnp.where(pair_of == jnp.int16(pair), moved, packed)
        return packed

    def col_copy(p, d):
        side = d - LEFT
        return pltpu.make_async_remote_copy(
            src_ref=stacks[p][side].at[1, pl.ds(ch, ch)], dst_ref=ghost.at[p, slot[d] - LEFT],
            send_sem=send_col.at[p, side], recv_sem=recv_col.at[p, slot[d] - LEFT], device_id=target[d], device_id_type=MESH)

    def col_wait(p, side):
        pltpu.make_async_copy(ghost.at[p, side], ghost.at[p, side], recv_col.at[p, side]).wait()

    def edge_copy(p, d):
        return pltpu.make_async_remote_copy(
            src_ref=pack_e.at[p], dst_ref=recv_e.at[p, slot[d]],
            send_sem=send_e.at[p, d], recv_sem=recv_e_sem.at[p, slot[d]], device_id=target[d], device_id_type=MESH)

    def edge_wait(p, d):
        pltpu.make_async_copy(recv_e.at[p, d], recv_e.at[p, d], recv_e_sem.at[p, d]).wait()

    def chunk_copy(p, k, d):
        return pltpu.make_async_remote_copy(
            src_ref=pack_c.at[p, k - 1], dst_ref=recv_c.at[p, k - 1, slot[d]],
            send_sem=send_c.at[p, k - 1, d], recv_sem=recv_c_sem.at[p, k - 1, slot[d]], device_id=target[d], device_id_type=MESH)

    def chunk_wait(p, k, d):
        pltpu.make_async_copy(recv_c.at[p, k - 1, d], recv_c.at[p, k - 1, d], recv_c_sem.at[p, k - 1, d]).wait()

    def send_cols(p):
        for d in (LEFT, RIGHT):
            at(d, lambda d=d: col_copy(p, d).start())

    def send_chunk(p, k):
        if k == 0:
            for d in EDGE_DIRS:
                at(d, lambda d=d: edge_copy(p, d).start())
        else:
            for d in (UP, DOWN):
                at(d, lambda d=d: chunk_copy(p, k, d).start())

    def wait_sends(p):
        for d in range(8):
            def wait_for(d=d):
                if d in (LEFT, RIGHT):
                    col_copy(p, d).wait_send()
                else:
                    edge_copy(p, d).wait_send()
                if d in (UP, DOWN):
                    for k in range(1, len(chunks)):
                        chunk_copy(p, k, d).wait_send()

            at(d, wait_for)

    def wait_recv(p, k):
        if k == 0:
            for d in (LEFT, RIGHT):
                at(d, lambda d=d: col_wait(p, d - LEFT))
            for d in EDGE_DIRS:
                at(d, lambda d=d: edge_wait(p, d))
        else:
            for d in (UP, DOWN):
                at(d, lambda d=d: chunk_wait(p, k, d))

    def halo(above, below):
        return jnp.where(even, above, below)

    def shifted(dst, s, h, edges, pair0):
        for g in range(groups):
            part = h[16 * g:16 * g + 16]
            edge = pltpu.roll(edges, (-(2 * (16 * g + pair0) + 1)) % lanes, 1)
            dst[s, pl.ds(16 * g, 16)] = pltpu.roll(jnp.where(last, edge, part), 1, 1)
            dst[s, pl.ds(2 * ch + 16 * g, 16)] = pltpu.roll(jnp.where(first, edge, part), lanes - 1, 1)

    def prepare_ghosts(p):
        for side, (up, down) in enumerate(((UP_LEFT, DOWN_LEFT), (UP_RIGHT, DOWN_RIGHT))):
            h = ghost[p, side]
            dst = stacks[p][side]
            dst[0, pl.ds(ch, ch)] = h
            shifted(dst, 0, h, halo(recv_e[p, up], recv_e[p, down]), 1 - side)

    def prepare(p, k):
        if k == 0:
            prepare_ghosts(p)
            edges = halo(recv_e[p, UP], recv_e[p, DOWN])
        else:
            edges = halo(recv_c[p, k - 1, UP], recv_c[p, k - 1, DOWN])
        for local, j in enumerate(chunks[k]):
            for side in range(2):
                dst = stacks[p][side]
                shifted(dst, j + 1, dst[j + 1, pl.ds(ch, ch)], edges, 2 * local + side)

    def matmul(p, j):
        left, right = stacks[p]
        flat = lambda ref, s: ref[s]
        l_next = flat(left, j + 2) if j + 1 < tiles else flat(right, tiles)
        r_next = flat(right, j + 2) if j + 1 < tiles else flat(left, tiles)
        stack_l = jnp.concatenate([flat(left, j), flat(left, j + 1), l_next], axis=0)
        stack_r = jnp.concatenate([r_next, flat(right, j + 1), flat(right, j)], axis=0)
        stack = jnp.concatenate([stack_l, stack_r], axis=1)
        return jnp.dot(w_ref[...], stack, preferred_element_type=jnp.float32)

    def update(side, j, gates):
        part = gates[:, side * lanes:(side + 1) * lanes] + bs[...]
        in_t, forget_t, out_t, cand = (part[ch * b:ch * b + ch] for b in range(4))
        c = (0.5 * jnp.tanh(forget_t) + 0.5) * cs[side, j] + (0.5 * jnp.tanh(in_t) + 0.5) * jnp.tanh(cand)
        cs[side, j] = c
        return ((0.5 * jnp.tanh(out_t) + 0.5) * jnp.tanh(c)).astype(jnp.bfloat16)

    def out_copy(p, t, side, j):
        return pltpu.make_async_copy(stacks[p][side].at[j + 1, pl.ds(ch, ch)], h_seq.at[t, column(side, j)], out_sem.at[p, side, j])

    def wait_outs(p):
        for side in range(2):
            for j in range(tiles):
                out_copy(p, 0, side, j).wait()

    def store_pack(p, k, packed):
        if k == 0:
            pack_e[p] = packed
        else:
            pack_c[p, k - 1] = packed

    def step(t, p):
        q = 1 - p
        line = bias_ref[pl.ds(t, 1), :]
        bs[...] = jnp.transpose(jnp.broadcast_to(line, (lanes, line.shape[1])))
        for k in range(2):
            wait_recv(p, k)
            prepare(p, k)
        ready = 1
        packed = zero
        for j in range(tiles):
            if j + 1 < tiles and chunk_of[j + 1][0] > ready:
                ready = chunk_of[j + 1][0]
                wait_recv(p, ready)
                prepare(p, ready)
            gates = matmul(p, j)
            k, local = chunk_of[j]
            for side in range(2):
                h = update(side, j, gates)
                stacks[q][side][j + 1, pl.ds(ch, ch)] = h
                packed = pack(packed, local, side, h)
            for side in range(2):
                out_copy(q, t, side, j).start()
            if j == 0:
                send_cols(q)
            if j == chunks[k][-1]:
                store_pack(q, k, packed)
                packed = zero
                send_chunk(q, k)
        wait_sends(p)

    for k, chunk in enumerate(chunks):
        packed = zero
        for local, j in enumerate(chunk):
            for side in range(2):
                packed = pack(packed, local, side, stacks[0][side][j + 1, pl.ds(ch, ch)])
        store_pack(0, k, packed)
        if k == 0:
            send_cols(0)
        send_chunk(0, k)

    def two_steps(i, carry):
        step(2 * i, 0)

        @pl.when(i > 0)
        def _():
            wait_outs(0)

        step(2 * i + 1, 1)
        wait_outs(1)
        return carry

    lax.fori_loop(0, steps // 2, two_steps, 0)
    for k in range(len(chunks)):
        wait_recv(0, k)
    wait_sends(0)
    wait_outs(0)
    stores = [pltpu.make_async_copy(cs.at[side, j], c_last.at[column(side, j)], init_sem.at[1, side, j]) for side in range(2) for j in range(tiles)]
    for copy in stores:
        copy.start()
    for copy in stores:
        copy.wait()


def solution(mesh):
    rows_n, cols_n = mesh.shape["rows"], mesh.shape["cols"]

    def device_fn(h_init, c_init, w_rec, gate_bias):
        _, height, width, ch = h_init.shape
        steps, gates_n = gate_bias.shape
        tiles = width // 2
        chunks = (tuple(range(1)), tuple(range(1, 6)), tuple(range(6, 11)), tuple(range(11, tiles)))
        scale = jnp.where(jnp.arange(gates_n) < 3 * ch, 0.5, 1.0).astype(jnp.float32)
        w = (jnp.transpose(w_rec, (3, 1, 0, 2)).reshape(gates_n, 9 * ch).astype(jnp.float32) * scale[:, None]).astype(jnp.bfloat16)
        bias = gate_bias * scale
        h_in = jnp.transpose(h_init[0], (1, 2, 0))
        c_in = jnp.transpose(c_init[0], (1, 2, 0))
        stack = pltpu.VMEM((tiles + 1, 3 * ch, height), jnp.bfloat16)
        any_spec = pl.BlockSpec(memory_space=pl.ANY)
        vmem_spec = pl.BlockSpec(memory_space=pltpu.VMEM)
        dma = pltpu.SemaphoreType.DMA
        h_seq, c_last = pl.pallas_call(
            functools.partial(kernel, steps, tiles, chunks, rows_n, cols_n),
            out_shape=(jax.ShapeDtypeStruct((steps, width, ch, height), jnp.bfloat16),
                       jax.ShapeDtypeStruct((width, ch, height), jnp.float32)),
            in_specs=[any_spec, any_spec, vmem_spec, vmem_spec],
            out_specs=(any_spec, any_spec),
            scratch_shapes=[
                stack, stack, stack, stack,
                pltpu.VMEM((2, tiles, ch, height), jnp.float32),
                pltpu.VMEM((gates_n, height), jnp.float32),
                pltpu.VMEM((2, 2, ch, height), jnp.bfloat16),
                pltpu.VMEM((2, 16, height), jnp.bfloat16),
                pltpu.VMEM((2, len(chunks) - 1, 16, height), jnp.bfloat16),
                pltpu.VMEM((2, 8, 16, height), jnp.bfloat16),
                pltpu.VMEM((2, len(chunks) - 1, 2, 16, height), jnp.bfloat16),
                dma((2, 2, tiles)), dma((2, 2, tiles)),
                dma((2, 2)), dma((2, 2)), dma((2, 8)), dma((2, 8)),
                dma((2, len(chunks) - 1, 2)), dma((2, len(chunks) - 1, 2)),
            ],
            compiler_params=pltpu.CompilerParams(collective_id=0, has_side_effects=True, vmem_limit_bytes=60 * 1024 * 1024),
        )(h_in, c_in, w, bias)
        return jnp.transpose(h_seq, (0, 3, 1, 2))[:, None], jnp.transpose(c_last, (2, 0, 1))[None]

    state_spec = P("dp", "rows", "cols", None)
    return jax.shard_map(device_fn, mesh=mesh, in_specs=(state_spec, state_spec, P(), P()), out_specs=(P(None, "dp", "rows", "cols", None), state_spec), check_vma=False)
```

```python
import functools

import jax
import jax.numpy as jnp
from jax import lax
from jax.experimental import pallas as pl
from jax.experimental.pallas import tpu as pltpu
from jax.sharding import PartitionSpec as P

UP, DOWN, LEFT, RIGHT, UP_LEFT, UP_RIGHT, DOWN_LEFT, DOWN_RIGHT = range(8)
OFFSETS = ((-1, 0), (1, 0), (0, -1), (0, 1), (-1, -1), (-1, 1), (1, -1), (1, 1))
OPPOSITE = (DOWN, UP, RIGHT, LEFT, DOWN_RIGHT, DOWN_LEFT, UP_RIGHT, UP_LEFT)
EDGE_DIRS = (UP, DOWN, UP_LEFT, UP_RIGHT, DOWN_LEFT, DOWN_RIGHT)
MESH = pl.DeviceIdType.MESH


def kernel(steps, tiles, chunks, rows_n, cols_n, h_init, c_init, w_ref, bias_ref, h_seq, c_last,
           hl0, hr0, hl1, hr1, cs, ws, bs, ghost, pack_e, pack_c, recv_e, recv_c,
           init_sem, out_sem, send_col, recv_col, send_e, recv_e_sem, send_c, recv_c_sem):
    ch, lanes = h_init.shape[1], h_init.shape[2]
    cols = 2 * tiles
    groups = ch // 16
    stacks = ((hl0, hr0), (hl1, hr1))
    row, col = lax.axis_index("rows"), lax.axis_index("cols")
    chunk_of = {j: (k, j - chunk[0]) for k, chunk in enumerate(chunks) for j in chunk}

    has, target, slot = [], [], []
    for d, (dr, dc) in enumerate(OFFSETS):
        r, c = row + dr, col + dc
        has.append((r >= 0) & (r < rows_n) & (c >= 0) & (c < cols_n))
        target.append({"rows": r, "cols": c})
        slot.append(OPPOSITE[d])

    def at(d, action):
        pl.when(has[d])(action)

    for ref in (ghost, recv_e, recv_c):
        ref[...] = jnp.zeros_like(ref)
    barrier = pltpu.get_barrier_semaphore()
    for d in range(8):
        at(d, lambda d=d: pl.semaphore_signal(barrier, inc=1, device_id=target[d], device_id_type=MESH))
    around_r = 1 + has[UP].astype(jnp.int32) + has[DOWN].astype(jnp.int32)
    around_c = 1 + has[LEFT].astype(jnp.int32) + has[RIGHT].astype(jnp.int32)
    pl.semaphore_wait(barrier, around_r * around_c - 1)

    def column(side, j):
        return j if side == 0 else cols - 1 - j

    loads = []
    for side in range(2):
        for j in range(tiles):
            loads.append(pltpu.make_async_copy(h_init.at[column(side, j)], stacks[0][side].at[j + 1, pl.ds(ch, ch)], init_sem.at[0, side, j]))
            loads.append(pltpu.make_async_copy(c_init.at[column(side, j)], cs.at[side, j], init_sem.at[1, side, j]))
    for copy in loads:
        copy.start()
    for copy in loads:
        copy.wait()

    ws[pl.ds(0, 3 * ch), :] = w_ref[pl.ds(0, 3 * ch), :] * jnp.bfloat16(0.5)
    ws[pl.ds(3 * ch, ch), :] = w_ref[pl.ds(3 * ch, ch), :]
    scale = jnp.where(lax.broadcasted_iota(jnp.int32, (1, 4 * ch), 1) < 3 * ch, 0.5, 1.0).astype(jnp.float32)
    lane = lax.broadcasted_iota(jnp.int16, (16, lanes), 1)
    pair_of = lax.shift_right_logical(lane, jnp.int16(1))
    even = (lane & jnp.int16(1)) == jnp.int16(0)
    first, last = lane == jnp.int16(0), lane == jnp.int16(lanes - 1)
    zero = jnp.zeros((16, lanes), jnp.bfloat16)

    def pack(packed, local, side, h):
        for g in range(groups):
            pair = 16 * g + 2 * local + side
            moved = pltpu.roll(h[16 * g:16 * g + 16], (1 + 2 * pair) % lanes, 1)
            packed = jnp.where(pair_of == jnp.int16(pair), moved, packed)
        return packed

    def col_copy(p, d):
        side = d - LEFT
        return pltpu.make_async_remote_copy(
            src_ref=stacks[p][side].at[1, pl.ds(ch, ch)], dst_ref=ghost.at[p, slot[d] - LEFT],
            send_sem=send_col.at[p, side], recv_sem=recv_col.at[p, slot[d] - LEFT], device_id=target[d], device_id_type=MESH)

    def col_wait(p, side):
        pltpu.make_async_copy(ghost.at[p, side], ghost.at[p, side], recv_col.at[p, side]).wait()

    def edge_copy(p, d):
        return pltpu.make_async_remote_copy(
            src_ref=pack_e.at[p], dst_ref=recv_e.at[p, slot[d]],
            send_sem=send_e.at[p, d], recv_sem=recv_e_sem.at[p, slot[d]], device_id=target[d], device_id_type=MESH)

    def edge_wait(p, d):
        pltpu.make_async_copy(recv_e.at[p, d], recv_e.at[p, d], recv_e_sem.at[p, d]).wait()

    def chunk_copy(p, k, d):
        return pltpu.make_async_remote_copy(
            src_ref=pack_c.at[p, k - 1], dst_ref=recv_c.at[p, k - 1, slot[d]],
            send_sem=send_c.at[p, k - 1, d], recv_sem=recv_c_sem.at[p, k - 1, slot[d]], device_id=target[d], device_id_type=MESH)

    def chunk_wait(p, k, d):
        pltpu.make_async_copy(recv_c.at[p, k - 1, d], recv_c.at[p, k - 1, d], recv_c_sem.at[p, k - 1, d]).wait()

    def send_cols(p):
        for d in (LEFT, RIGHT):
            at(d, lambda d=d: col_copy(p, d).start())

    def send_chunk(p, k):
        if k == 0:
            for d in EDGE_DIRS:
                at(d, lambda d=d: edge_copy(p, d).start())
        else:
            for d in (UP, DOWN):
                at(d, lambda d=d: chunk_copy(p, k, d).start())

    def wait_sends(p):
        for d in range(8):
            def wait_for(d=d):
                if d in (LEFT, RIGHT):
                    col_copy(p, d).wait_send()
                else:
                    edge_copy(p, d).wait_send()
                if d in (UP, DOWN):
                    for k in range(1, len(chunks)):
                        chunk_copy(p, k, d).wait_send()

            at(d, wait_for)

    def wait_recv(p, k):
        if k == 0:
            for d in (LEFT, RIGHT):
                at(d, lambda d=d: col_wait(p, d - LEFT))
            for d in EDGE_DIRS:
                at(d, lambda d=d: edge_wait(p, d))
        else:
            for d in (UP, DOWN):
                at(d, lambda d=d: chunk_wait(p, k, d))

    def halo(above, below):
        return jnp.where(even, above, below)

    def shifted(dst, s, h, edges, pair0):
        for g in range(groups):
            part = h[16 * g:16 * g + 16]
            edge = pltpu.roll(edges, (-(2 * (16 * g + pair0) + 1)) % lanes, 1)
            dst[s, pl.ds(16 * g, 16)] = pltpu.roll(jnp.where(last, edge, part), 1, 1)
            dst[s, pl.ds(2 * ch + 16 * g, 16)] = pltpu.roll(jnp.where(first, edge, part), lanes - 1, 1)

    def prepare_ghosts(p):
        for side, (up, down) in enumerate(((UP_LEFT, DOWN_LEFT), (UP_RIGHT, DOWN_RIGHT))):
            h = ghost[p, side]
            dst = stacks[p][side]
            dst[0, pl.ds(ch, ch)] = h
            shifted(dst, 0, h, halo(recv_e[p, up], recv_e[p, down]), 1 - side)

    def prepare(p, k):
        if k == 0:
            prepare_ghosts(p)
            edges = halo(recv_e[p, UP], recv_e[p, DOWN])
        else:
            edges = halo(recv_c[p, k - 1, UP], recv_c[p, k - 1, DOWN])
        for local, j in enumerate(chunks[k]):
            for side in range(2):
                dst = stacks[p][side]
                shifted(dst, j + 1, dst[j + 1, pl.ds(ch, ch)], edges, 2 * local + side)

    def matmul(p, j):
        left, right = stacks[p]
        flat = lambda ref, s: ref[s]
        l_next = flat(left, j + 2) if j + 1 < tiles else flat(right, tiles)
        r_next = flat(right, j + 2) if j + 1 < tiles else flat(left, tiles)
        stack_l = jnp.concatenate([flat(left, j), flat(left, j + 1), l_next], axis=0)
        stack_r = jnp.concatenate([r_next, flat(right, j + 1), flat(right, j)], axis=0)
        stack = jnp.concatenate([stack_l, stack_r], axis=1)
        return jnp.dot(ws[...], stack, preferred_element_type=jnp.float32)

    def update(side, j, gates):
        part = gates[:, side * lanes:(side + 1) * lanes] + bs[...]
        in_t, forget_t, out_t, cand = (part[ch * b:ch * b + ch] for b in range(4))
        c = (0.5 * jnp.tanh(forget_t) + 0.5) * cs[side, j] + (0.5 * jnp.tanh(in_t) + 0.5) * jnp.tanh(cand)
        cs[side, j] = c
        return ((0.5 * jnp.tanh(out_t) + 0.5) * jnp.tanh(c)).astype(jnp.bfloat16)

    def out_copy(p, t, side, j):
        return pltpu.make_async_copy(stacks[p][side].at[j + 1, pl.ds(ch, ch)], h_seq.at[t, column(side, j)], out_sem.at[p, side, j])

    def wait_outs(p):
        for side in range(2):
            for j in range(tiles):
                out_copy(p, 0, side, j).wait()

    def store_pack(p, k, packed):
        if k == 0:
            pack_e[p] = packed
        else:
            pack_c[p, k - 1] = packed

    def step(t, p):
        q = 1 - p
        line = bias_ref[pl.ds(t, 1), :] * scale
        bs[...] = jnp.transpose(jnp.broadcast_to(line, (lanes, line.shape[1])))
        for k in range(2):
            wait_recv(p, k)
            prepare(p, k)
        ready = 1
        packed = zero
        for j in range(tiles):
            if j + 1 < tiles and chunk_of[j + 1][0] > ready:
                ready = chunk_of[j + 1][0]
                wait_recv(p, ready)
                prepare(p, ready)
            gates = matmul(p, j)
            k, local = chunk_of[j]
            for side in range(2):
                h = update(side, j, gates)
                stacks[q][side][j + 1, pl.ds(ch, ch)] = h
                packed = pack(packed, local, side, h)
            for side in range(2):
                out_copy(q, t, side, j).start()
            if j == 0:
                send_cols(q)
            if j == chunks[k][-1]:
                store_pack(q, k, packed)
                packed = zero
                send_chunk(q, k)
        wait_sends(p)

    for k, chunk in enumerate(chunks):
        packed = zero
        for local, j in enumerate(chunk):
            for side in range(2):
                packed = pack(packed, local, side, stacks[0][side][j + 1, pl.ds(ch, ch)])
        store_pack(0, k, packed)
        if k == 0:
            send_cols(0)
        send_chunk(0, k)

    def two_steps(i, carry):
        step(2 * i, 0)

        @pl.when(i > 0)
        def _():
            wait_outs(0)

        step(2 * i + 1, 1)
        wait_outs(1)
        return carry

    lax.fori_loop(0, steps // 2, two_steps, 0)
    for k in range(len(chunks)):
        wait_recv(0, k)
    wait_sends(0)
    wait_outs(0)
    stores = [pltpu.make_async_copy(cs.at[side, j], c_last.at[column(side, j)], init_sem.at[1, side, j]) for side in range(2) for j in range(tiles)]
    for copy in stores:
        copy.start()
    for copy in stores:
        copy.wait()


def solution(mesh):
    rows_n, cols_n = mesh.shape["rows"], mesh.shape["cols"]

    def device_fn(h_init, c_init, w_rec, gate_bias):
        _, height, width, ch = h_init.shape
        steps, gates_n = gate_bias.shape
        tiles = width // 2
        chunks = (tuple(range(1)), tuple(range(1, tiles // 2)), tuple(range(tiles // 2, tiles)))
        w = jnp.transpose(w_rec, (3, 1, 0, 2)).reshape(gates_n, 9 * ch)
        h_in = jnp.transpose(h_init[0], (1, 2, 0))
        c_in = jnp.transpose(c_init[0], (1, 2, 0))
        stack = pltpu.VMEM((tiles + 1, 3 * ch, height), jnp.bfloat16)
        any_spec = pl.BlockSpec(memory_space=pl.ANY)
        vmem_spec = pl.BlockSpec(memory_space=pltpu.VMEM)
        dma = pltpu.SemaphoreType.DMA
        h_seq, c_last = pl.pallas_call(
            functools.partial(kernel, steps, tiles, chunks, rows_n, cols_n),
            out_shape=(jax.ShapeDtypeStruct((steps, width, ch, height), jnp.bfloat16),
                       jax.ShapeDtypeStruct((width, ch, height), jnp.float32)),
            in_specs=[any_spec, any_spec, vmem_spec, vmem_spec],
            out_specs=(any_spec, any_spec),
            scratch_shapes=[
                stack, stack, stack, stack,
                pltpu.VMEM((2, tiles, ch, height), jnp.float32),
                pltpu.VMEM((gates_n, 9 * ch), jnp.bfloat16),
                pltpu.VMEM((gates_n, height), jnp.float32),
                pltpu.VMEM((2, 2, ch, height), jnp.bfloat16),
                pltpu.VMEM((2, 16, height), jnp.bfloat16),
                pltpu.VMEM((2, len(chunks) - 1, 16, height), jnp.bfloat16),
                pltpu.VMEM((2, 8, 16, height), jnp.bfloat16),
                pltpu.VMEM((2, len(chunks) - 1, 2, 16, height), jnp.bfloat16),
                dma((2, 2, tiles)), dma((2, 2, tiles)),
                dma((2, 2)), dma((2, 2)), dma((2, 8)), dma((2, 8)),
                dma((2, len(chunks) - 1, 2)), dma((2, len(chunks) - 1, 2)),
            ],
            compiler_params=pltpu.CompilerParams(collective_id=0, has_side_effects=True, vmem_limit_bytes=60 * 1024 * 1024),
        )(h_in, c_in, w, gate_bias)
        return jnp.transpose(h_seq, (0, 3, 1, 2))[:, None], jnp.transpose(c_last, (2, 0, 1))[None]

    state_spec = P("dp", "rows", "cols", None)
    return jax.shard_map(device_fn, mesh=mesh, in_specs=(state_spec, state_spec, P(), P()), out_specs=(P(None, "dp", "rows", "cols", None), state_spec), check_vma=False)
```

```python
import functools

import jax
import jax.numpy as jnp
from jax import lax
from jax.experimental import pallas as pl
from jax.experimental.pallas import tpu as pltpu
from jax.sharding import PartitionSpec as P

UP, DOWN, LEFT, RIGHT, UP_LEFT, UP_RIGHT, DOWN_LEFT, DOWN_RIGHT = range(8)
OFFSETS = ((-1, 0), (1, 0), (0, -1), (0, 1), (-1, -1), (-1, 1), (1, -1), (1, 1))
OPPOSITE = (DOWN, UP, RIGHT, LEFT, DOWN_RIGHT, DOWN_LEFT, UP_RIGHT, UP_LEFT)
EDGE_DIRS = (UP, DOWN, UP_LEFT, UP_RIGHT, DOWN_LEFT, DOWN_RIGHT)
MESH = pl.DeviceIdType.MESH


def kernel(steps, tiles, chunks, rows_n, cols_n, h_init, c_init, w_ref, bias_ref, h_seq, c_last,
           hl0, hr0, hl1, hr1, cs, ws, bs, ghost, pack_e, pack_c, recv_e, recv_c,
           init_sem, out_sem, send_col, recv_col, send_e, recv_e_sem, send_c, recv_c_sem):
    ch, lanes = h_init.shape[1], h_init.shape[2]
    cols = 2 * tiles
    groups = ch // 16
    stacks = ((hl0, hr0), (hl1, hr1))
    row, col = lax.axis_index("rows"), lax.axis_index("cols")
    chunk_of = {j: (k, j - chunk[0]) for k, chunk in enumerate(chunks) for j in chunk}

    has, target, slot = [], [], []
    for d, (dr, dc) in enumerate(OFFSETS):
        r, c = row + dr, col + dc
        has.append((r >= 0) & (r < rows_n) & (c >= 0) & (c < cols_n))
        target.append({"rows": r, "cols": c})
        slot.append(OPPOSITE[d])

    def at(d, action, live=None):
        pl.when(has[d] if live is None else has[d] & live)(action)

    for ref in (ghost, recv_e, recv_c):
        ref[...] = jnp.zeros_like(ref)
    barrier = pltpu.get_barrier_semaphore()
    for d in range(8):
        at(d, lambda d=d: pl.semaphore_signal(barrier, inc=1, device_id=target[d], device_id_type=MESH))
    around_r = 1 + has[UP].astype(jnp.int32) + has[DOWN].astype(jnp.int32)
    around_c = 1 + has[LEFT].astype(jnp.int32) + has[RIGHT].astype(jnp.int32)
    pl.semaphore_wait(barrier, around_r * around_c - 1)

    def column(side, j):
        return j if side == 0 else cols - 1 - j

    loads = []
    for side in range(2):
        for j in range(tiles):
            loads.append(pltpu.make_async_copy(h_init.at[column(side, j)], stacks[0][side].at[j + 1, pl.ds(ch, ch)], init_sem.at[0, side, j]))
            loads.append(pltpu.make_async_copy(c_init.at[column(side, j)], cs.at[side, j], init_sem.at[1, side, j]))
    for copy in loads:
        copy.start()
    for copy in loads:
        copy.wait()

    ws[pl.ds(0, 3 * ch), :] = w_ref[pl.ds(0, 3 * ch), :] * jnp.bfloat16(0.5)
    ws[pl.ds(3 * ch, ch), :] = w_ref[pl.ds(3 * ch, ch), :]
    scale = jnp.where(lax.broadcasted_iota(jnp.int32, (1, 4 * ch), 1) < 3 * ch, 0.5, 1.0).astype(jnp.float32)
    lane = lax.broadcasted_iota(jnp.int16, (16, lanes), 1)
    pair_of = lax.shift_right_logical(lane, jnp.int16(1))
    even = (lane & jnp.int16(1)) == jnp.int16(0)
    first, last = lane == jnp.int16(0), lane == jnp.int16(lanes - 1)
    zero = jnp.zeros((16, lanes), jnp.bfloat16)

    def pack(packed, local, side, h):
        for g in range(groups):
            pair = 16 * g + 2 * local + side
            moved = pltpu.roll(h[16 * g:16 * g + 16], (1 + 2 * pair) % lanes, 1)
            packed = jnp.where(pair_of == jnp.int16(pair), moved, packed)
        return packed

    def col_copy(p, d):
        side = d - LEFT
        return pltpu.make_async_remote_copy(
            src_ref=stacks[p][side].at[1, pl.ds(ch, ch)], dst_ref=ghost.at[p, slot[d] - LEFT],
            send_sem=send_col.at[p, side], recv_sem=recv_col.at[p, slot[d] - LEFT], device_id=target[d], device_id_type=MESH)

    def col_wait(p, side):
        pltpu.make_async_copy(ghost.at[p, side], ghost.at[p, side], recv_col.at[p, side]).wait()

    def edge_copy(p, d):
        return pltpu.make_async_remote_copy(
            src_ref=pack_e.at[p], dst_ref=recv_e.at[p, slot[d]],
            send_sem=send_e.at[p, d], recv_sem=recv_e_sem.at[p, slot[d]], device_id=target[d], device_id_type=MESH)

    def edge_wait(p, d):
        pltpu.make_async_copy(recv_e.at[p, d], recv_e.at[p, d], recv_e_sem.at[p, d]).wait()

    def chunk_copy(p, k, d):
        return pltpu.make_async_remote_copy(
            src_ref=pack_c.at[p, k - 1], dst_ref=recv_c.at[p, k - 1, slot[d]],
            send_sem=send_c.at[p, k - 1, d], recv_sem=recv_c_sem.at[p, k - 1, slot[d]], device_id=target[d], device_id_type=MESH)

    def chunk_wait(p, k, d):
        pltpu.make_async_copy(recv_c.at[p, k - 1, d], recv_c.at[p, k - 1, d], recv_c_sem.at[p, k - 1, d]).wait()

    def send_cols(p, live=None):
        for d in (LEFT, RIGHT):
            at(d, lambda d=d: col_copy(p, d).start(), live)

    def send_chunk(p, k, live=None):
        if k == 0:
            for d in EDGE_DIRS:
                at(d, lambda d=d: edge_copy(p, d).start(), live)
        else:
            for d in (UP, DOWN):
                at(d, lambda d=d: chunk_copy(p, k, d).start(), live)

    def wait_sends(p):
        for d in range(8):
            def wait_for(d=d):
                if d in (LEFT, RIGHT):
                    col_copy(p, d).wait_send()
                else:
                    edge_copy(p, d).wait_send()
                if d in (UP, DOWN):
                    for k in range(1, len(chunks)):
                        chunk_copy(p, k, d).wait_send()

            at(d, wait_for)

    def wait_recv(p, k):
        if k == 0:
            for d in (LEFT, RIGHT):
                at(d, lambda d=d: col_wait(p, d - LEFT))
            for d in EDGE_DIRS:
                at(d, lambda d=d: edge_wait(p, d))
        else:
            for d in (UP, DOWN):
                at(d, lambda d=d: chunk_wait(p, k, d))

    def halo(above, below):
        return jnp.where(even, above, below)

    def shifted(dst, s, h, edges, pair0):
        for g in range(groups):
            part = h[16 * g:16 * g + 16]
            edge = pltpu.roll(edges, (-(2 * (16 * g + pair0) + 1)) % lanes, 1)
            dst[s, pl.ds(16 * g, 16)] = pltpu.roll(jnp.where(last, edge, part), 1, 1)
            dst[s, pl.ds(2 * ch + 16 * g, 16)] = pltpu.roll(jnp.where(first, edge, part), lanes - 1, 1)

    def prepare_ghosts(p):
        for side, (up, down) in enumerate(((UP_LEFT, DOWN_LEFT), (UP_RIGHT, DOWN_RIGHT))):
            h = ghost[p, side]
            dst = stacks[p][side]
            dst[0, pl.ds(ch, ch)] = h
            shifted(dst, 0, h, halo(recv_e[p, up], recv_e[p, down]), 1 - side)

    def prepare(p, k):
        if k == 0:
            prepare_ghosts(p)
            edges = halo(recv_e[p, UP], recv_e[p, DOWN])
        else:
            edges = halo(recv_c[p, k - 1, UP], recv_c[p, k - 1, DOWN])
        for local, j in enumerate(chunks[k]):
            for side in range(2):
                dst = stacks[p][side]
                shifted(dst, j + 1, dst[j + 1, pl.ds(ch, ch)], edges, 2 * local + side)

    def matmul(p, j):
        left, right = stacks[p]
        flat = lambda ref, s: ref[s]
        l_next = flat(left, j + 2) if j + 1 < tiles else flat(right, tiles)
        r_next = flat(right, j + 2) if j + 1 < tiles else flat(left, tiles)
        stack_l = jnp.concatenate([flat(left, j), flat(left, j + 1), l_next], axis=0)
        stack_r = jnp.concatenate([r_next, flat(right, j + 1), flat(right, j)], axis=0)
        stack = jnp.concatenate([stack_l, stack_r], axis=1)
        return jnp.dot(ws[...], stack, preferred_element_type=jnp.float32)

    def update(side, j, gates):
        part = gates[:, side * lanes:(side + 1) * lanes] + bs[...]
        in_t, forget_t, out_t, cand = (part[ch * b:ch * b + ch] for b in range(4))
        c = (0.5 * jnp.tanh(forget_t) + 0.5) * cs[side, j] + (0.5 * jnp.tanh(in_t) + 0.5) * jnp.tanh(cand)
        cs[side, j] = c
        return ((0.5 * jnp.tanh(out_t) + 0.5) * jnp.tanh(c)).astype(jnp.bfloat16)

    def out_copy(p, t, side, j):
        return pltpu.make_async_copy(stacks[p][side].at[j + 1, pl.ds(ch, ch)], h_seq.at[t, column(side, j)], out_sem.at[p, side, j])

    def wait_outs(p):
        for side in range(2):
            for j in range(tiles):
                out_copy(p, 0, side, j).wait()

    def store_pack(p, k, packed):
        if k == 0:
            pack_e[p] = packed
        else:
            pack_c[p, k - 1] = packed

    def step(t, p):
        q = 1 - p
        live = t < steps - 1 if p else None
        line = bias_ref[pl.ds(t, 1), :] * scale
        bs[...] = jnp.transpose(jnp.broadcast_to(line, (lanes, line.shape[1])))
        for k in range(2):
            wait_recv(p, k)
            prepare(p, k)
        ready = 1
        packed = zero
        for j in range(tiles):
            if j + 1 < tiles and chunk_of[j + 1][0] > ready:
                ready = chunk_of[j + 1][0]
                wait_recv(p, ready)
                prepare(p, ready)
            gates = matmul(p, j)
            k, local = chunk_of[j]
            for side in range(2):
                h = update(side, j, gates)
                stacks[q][side][j + 1, pl.ds(ch, ch)] = h
                packed = pack(packed, local, side, h)
            for side in range(2):
                out_copy(q, t, side, j).start()
            if j == 0:
                send_cols(q, live)
            if j == chunks[k][-1]:
                store_pack(q, k, packed)
                packed = zero
                send_chunk(q, k, live)
        wait_sends(p)

    for k, chunk in enumerate(chunks):
        packed = zero
        for local, j in enumerate(chunk):
            for side in range(2):
                packed = pack(packed, local, side, stacks[0][side][j + 1, pl.ds(ch, ch)])
        store_pack(0, k, packed)
        if k == 0:
            send_cols(0)
        send_chunk(0, k)

    def two_steps(i, carry):
        step(2 * i, 0)

        @pl.when(i > 0)
        def _():
            wait_outs(0)

        step(2 * i + 1, 1)
        wait_outs(1)
        return carry

    lax.fori_loop(0, steps // 2, two_steps, 0)
    wait_outs(0)
    stores = [pltpu.make_async_copy(cs.at[side, j], c_last.at[column(side, j)], init_sem.at[1, side, j]) for side in range(2) for j in range(tiles)]
    for copy in stores:
        copy.start()
    for copy in stores:
        copy.wait()


def solution(mesh):
    rows_n, cols_n = mesh.shape["rows"], mesh.shape["cols"]

    def device_fn(h_init, c_init, w_rec, gate_bias):
        _, height, width, ch = h_init.shape
        steps, gates_n = gate_bias.shape
        tiles = width // 2
        chunks = (tuple(range(1)), tuple(range(1, tiles // 2)), tuple(range(tiles // 2, tiles)))
        w = jnp.transpose(w_rec, (3, 1, 0, 2)).reshape(gates_n, 9 * ch)
        h_in = jnp.transpose(h_init[0], (1, 2, 0))
        c_in = jnp.transpose(c_init[0], (1, 2, 0))
        stack = pltpu.VMEM((tiles + 1, 3 * ch, height), jnp.bfloat16)
        any_spec = pl.BlockSpec(memory_space=pl.ANY)
        vmem_spec = pl.BlockSpec(memory_space=pltpu.VMEM)
        dma = pltpu.SemaphoreType.DMA
        h_seq, c_last = pl.pallas_call(
            functools.partial(kernel, steps, tiles, chunks, rows_n, cols_n),
            out_shape=(jax.ShapeDtypeStruct((steps, width, ch, height), jnp.bfloat16),
                       jax.ShapeDtypeStruct((width, ch, height), jnp.float32)),
            in_specs=[any_spec, any_spec, vmem_spec, vmem_spec],
            out_specs=(any_spec, any_spec),
            scratch_shapes=[
                stack, stack, stack, stack,
                pltpu.VMEM((2, tiles, ch, height), jnp.float32),
                pltpu.VMEM((gates_n, 9 * ch), jnp.bfloat16),
                pltpu.VMEM((gates_n, height), jnp.float32),
                pltpu.VMEM((2, 2, ch, height), jnp.bfloat16),
                pltpu.VMEM((2, 16, height), jnp.bfloat16),
                pltpu.VMEM((2, len(chunks) - 1, 16, height), jnp.bfloat16),
                pltpu.VMEM((2, 8, 16, height), jnp.bfloat16),
                pltpu.VMEM((2, len(chunks) - 1, 2, 16, height), jnp.bfloat16),
                dma((2, 2, tiles)), dma((2, 2, tiles)),
                dma((2, 2)), dma((2, 2)), dma((2, 8)), dma((2, 8)),
                dma((2, len(chunks) - 1, 2)), dma((2, len(chunks) - 1, 2)),
            ],
            compiler_params=pltpu.CompilerParams(collective_id=0, has_side_effects=True, vmem_limit_bytes=12 * 1024 * 1024),
        )(h_in, c_in, w, gate_bias)
        return jnp.transpose(h_seq, (0, 3, 1, 2))[:, None], jnp.transpose(c_last, (2, 0, 1))[None]

    state_spec = P("dp", "rows", "cols", None)
    return jax.shard_map(device_fn, mesh=mesh, in_specs=(state_spec, state_spec, P(), P()), out_specs=(P(None, "dp", "rows", "cols", None), state_spec), check_vma=False)
```

```python
import functools

import jax
import jax.numpy as jnp
from jax import lax
from jax.experimental import pallas as pl
from jax.experimental.pallas import tpu as pltpu
from jax.sharding import PartitionSpec as P

UP, DOWN, LEFT, RIGHT, UP_LEFT, UP_RIGHT, DOWN_LEFT, DOWN_RIGHT = range(8)
OFFSETS = ((-1, 0), (1, 0), (0, -1), (0, 1), (-1, -1), (-1, 1), (1, -1), (1, 1))
OPPOSITE = (DOWN, UP, RIGHT, LEFT, DOWN_RIGHT, DOWN_LEFT, UP_RIGHT, UP_LEFT)
EDGE_DIRS = (UP, DOWN, UP_LEFT, UP_RIGHT, DOWN_LEFT, DOWN_RIGHT)
MESH = pl.DeviceIdType.MESH


def kernel(steps, tiles, chunks, rows_n, cols_n, h_init, c_init, w_ref, bias_ref, h_seq, c_last,
           hl0, hr0, hl1, hr1, ws, bs, ghost, pack_e, pack_c, recv_e, recv_c,
           send_col, recv_col, send_e, recv_e_sem, send_c, recv_c_sem):
    ch, lanes = h_init.shape[1], h_init.shape[2]
    cols = 2 * tiles
    groups = ch // 16
    stacks = ((hl0, hr0), (hl1, hr1))
    row, col = lax.axis_index("rows"), lax.axis_index("cols")
    chunk_of = {j: (k, j - chunk[0]) for k, chunk in enumerate(chunks) for j in chunk}

    has, target, slot = [], [], []
    for d, (dr, dc) in enumerate(OFFSETS):
        r, c = row + dr, col + dc
        has.append((r >= 0) & (r < rows_n) & (c >= 0) & (c < cols_n))
        target.append({"rows": r, "cols": c})
        slot.append(OPPOSITE[d])

    def at(d, action, live=None):
        pl.when(has[d] if live is None else has[d] & live)(action)

    for ref in (ghost, recv_e, recv_c):
        ref[...] = jnp.zeros_like(ref)
    barrier = pltpu.get_barrier_semaphore()
    for d in range(8):
        at(d, lambda d=d: pl.semaphore_signal(barrier, inc=1, device_id=target[d], device_id_type=MESH))
    around_r = 1 + has[UP].astype(jnp.int32) + has[DOWN].astype(jnp.int32)
    around_c = 1 + has[LEFT].astype(jnp.int32) + has[RIGHT].astype(jnp.int32)
    pl.semaphore_wait(barrier, around_r * around_c - 1)

    def column(side, j):
        return j if side == 0 else cols - 1 - j

    for side in range(2):
        for j in range(tiles):
            stacks[0][side][j + 1, pl.ds(ch, ch)] = h_init[column(side, j)]
    c_last[...] = c_init[...]

    ws[pl.ds(0, 3 * ch), :] = w_ref[pl.ds(0, 3 * ch), :] * jnp.bfloat16(0.5)
    ws[pl.ds(3 * ch, ch), :] = w_ref[pl.ds(3 * ch, ch), :]
    scale = jnp.where(lax.broadcasted_iota(jnp.int32, (1, 4 * ch), 1) < 3 * ch, 0.5, 1.0).astype(jnp.float32)
    lane = lax.broadcasted_iota(jnp.int16, (16, lanes), 1)
    pair_of = lax.shift_right_logical(lane, jnp.int16(1))
    even = (lane & jnp.int16(1)) == jnp.int16(0)
    first, last = lane == jnp.int16(0), lane == jnp.int16(lanes - 1)
    zero = jnp.zeros((16, lanes), jnp.bfloat16)

    def pack(packed, local, side, h):
        for g in range(groups):
            pair = 16 * g + 2 * local + side
            moved = pltpu.roll(h[16 * g:16 * g + 16], (1 + 2 * pair) % lanes, 1)
            packed = jnp.where(pair_of == jnp.int16(pair), moved, packed)
        return packed

    def col_copy(p, d):
        side = d - LEFT
        return pltpu.make_async_remote_copy(
            src_ref=stacks[p][side].at[1, pl.ds(ch, ch)], dst_ref=ghost.at[p, slot[d] - LEFT],
            send_sem=send_col.at[p, side], recv_sem=recv_col.at[p, slot[d] - LEFT], device_id=target[d], device_id_type=MESH)

    def col_wait(p, side):
        pltpu.make_async_copy(ghost.at[p, side], ghost.at[p, side], recv_col.at[p, side]).wait()

    def edge_copy(p, d):
        return pltpu.make_async_remote_copy(
            src_ref=pack_e.at[p], dst_ref=recv_e.at[p, slot[d]],
            send_sem=send_e.at[p, d], recv_sem=recv_e_sem.at[p, slot[d]], device_id=target[d], device_id_type=MESH)

    def edge_wait(p, d):
        pltpu.make_async_copy(recv_e.at[p, d], recv_e.at[p, d], recv_e_sem.at[p, d]).wait()

    def chunk_copy(p, k, d):
        return pltpu.make_async_remote_copy(
            src_ref=pack_c.at[p, k - 1], dst_ref=recv_c.at[p, k - 1, slot[d]],
            send_sem=send_c.at[p, k - 1, d], recv_sem=recv_c_sem.at[p, k - 1, slot[d]], device_id=target[d], device_id_type=MESH)

    def chunk_wait(p, k, d):
        pltpu.make_async_copy(recv_c.at[p, k - 1, d], recv_c.at[p, k - 1, d], recv_c_sem.at[p, k - 1, d]).wait()

    def send_cols(p, live=None):
        for d in (LEFT, RIGHT):
            at(d, lambda d=d: col_copy(p, d).start(), live)

    def send_chunk(p, k, live=None):
        if k == 0:
            for d in EDGE_DIRS:
                at(d, lambda d=d: edge_copy(p, d).start(), live)
        else:
            for d in (UP, DOWN):
                at(d, lambda d=d: chunk_copy(p, k, d).start(), live)

    def wait_sends(p):
        for d in range(8):
            def wait_for(d=d):
                if d in (LEFT, RIGHT):
                    col_copy(p, d).wait_send()
                else:
                    edge_copy(p, d).wait_send()
                if d in (UP, DOWN):
                    for k in range(1, len(chunks)):
                        chunk_copy(p, k, d).wait_send()

            at(d, wait_for)

    def wait_recv(p, k):
        if k == 0:
            for d in (LEFT, RIGHT):
                at(d, lambda d=d: col_wait(p, d - LEFT))
            for d in EDGE_DIRS:
                at(d, lambda d=d: edge_wait(p, d))
        else:
            for d in (UP, DOWN):
                at(d, lambda d=d: chunk_wait(p, k, d))

    def halo(above, below):
        return jnp.where(even, above, below)

    def shifted(dst, s, h, edges, pair0):
        for g in range(groups):
            part = h[16 * g:16 * g + 16]
            edge = pltpu.roll(edges, (-(2 * (16 * g + pair0) + 1)) % lanes, 1)
            dst[s, pl.ds(16 * g, 16)] = pltpu.roll(jnp.where(last, edge, part), 1, 1)
            dst[s, pl.ds(2 * ch + 16 * g, 16)] = pltpu.roll(jnp.where(first, edge, part), lanes - 1, 1)

    def prepare_ghosts(p):
        for side, (up, down) in enumerate(((UP_LEFT, DOWN_LEFT), (UP_RIGHT, DOWN_RIGHT))):
            h = ghost[p, side]
            dst = stacks[p][side]
            dst[0, pl.ds(ch, ch)] = h
            shifted(dst, 0, h, halo(recv_e[p, up], recv_e[p, down]), 1 - side)

    def prepare(p, k):
        if k == 0:
            prepare_ghosts(p)
            edges = halo(recv_e[p, UP], recv_e[p, DOWN])
        else:
            edges = halo(recv_c[p, k - 1, UP], recv_c[p, k - 1, DOWN])
        for local, j in enumerate(chunks[k]):
            for side in range(2):
                dst = stacks[p][side]
                shifted(dst, j + 1, dst[j + 1, pl.ds(ch, ch)], edges, 2 * local + side)

    def matmul(p, j):
        left, right = stacks[p]
        flat = lambda ref, s: ref[s]
        l_next = flat(left, j + 2) if j + 1 < tiles else flat(right, tiles)
        r_next = flat(right, j + 2) if j + 1 < tiles else flat(left, tiles)
        stack_l = jnp.concatenate([flat(left, j), flat(left, j + 1), l_next], axis=0)
        stack_r = jnp.concatenate([r_next, flat(right, j + 1), flat(right, j)], axis=0)
        stack = jnp.concatenate([stack_l, stack_r], axis=1)
        return jnp.dot(ws[...], stack, preferred_element_type=jnp.float32)

    def update(side, j, gates):
        part = gates[:, side * lanes:(side + 1) * lanes] + bs[...]
        in_t, forget_t, out_t, cand = (part[ch * b:ch * b + ch] for b in range(4))
        c = (0.5 * jnp.tanh(forget_t) + 0.5) * c_last[column(side, j)] + (0.5 * jnp.tanh(in_t) + 0.5) * jnp.tanh(cand)
        c_last[column(side, j)] = c
        return ((0.5 * jnp.tanh(out_t) + 0.5) * jnp.tanh(c)).astype(jnp.bfloat16)

    def store_pack(p, k, packed):
        if k == 0:
            pack_e[p] = packed
        else:
            pack_c[p, k - 1] = packed

    def step(t, p):
        q = 1 - p
        live = t < steps - 1 if p else None
        line = bias_ref[pl.ds(t, 1), :] * scale
        bs[...] = jnp.transpose(jnp.broadcast_to(line, (lanes, line.shape[1])))
        for k in range(2):
            wait_recv(p, k)
            prepare(p, k)
        ready = 1
        packed = zero
        for j in range(tiles):
            if j + 1 < tiles and chunk_of[j + 1][0] > ready:
                ready = chunk_of[j + 1][0]
                wait_recv(p, ready)
                prepare(p, ready)
            gates = matmul(p, j)
            k, local = chunk_of[j]
            for side in range(2):
                h = update(side, j, gates)
                stacks[q][side][j + 1, pl.ds(ch, ch)] = h
                h_seq[t, column(side, j)] = h
                packed = pack(packed, local, side, h)
            if j == 0:
                send_cols(q, live)
            if j == chunks[k][-1]:
                store_pack(q, k, packed)
                packed = zero
                send_chunk(q, k, live)
        wait_sends(p)

    for k, chunk in enumerate(chunks):
        packed = zero
        for local, j in enumerate(chunk):
            for side in range(2):
                packed = pack(packed, local, side, stacks[0][side][j + 1, pl.ds(ch, ch)])
        store_pack(0, k, packed)
        if k == 0:
            send_cols(0)
        send_chunk(0, k)

    def two_steps(i, carry):
        step(2 * i, 0)
        step(2 * i + 1, 1)
        return carry

    lax.fori_loop(0, steps // 2, two_steps, 0)


def solution(mesh):
    rows_n, cols_n = mesh.shape["rows"], mesh.shape["cols"]

    def device_fn(h_init, c_init, w_rec, gate_bias):
        _, height, width, ch = h_init.shape
        steps, gates_n = gate_bias.shape
        tiles = width // 2
        chunks = (tuple(range(1)), tuple(range(1, tiles // 2)), tuple(range(tiles // 2, tiles)))
        w = jnp.transpose(w_rec, (3, 1, 0, 2)).reshape(gates_n, 9 * ch)
        h_in = jnp.transpose(h_init[0], (1, 2, 0))
        c_in = jnp.transpose(c_init[0], (1, 2, 0))
        stack = pltpu.VMEM((tiles + 1, 3 * ch, height), jnp.bfloat16)
        vmem_spec = pl.BlockSpec(memory_space=pltpu.VMEM)
        dma = pltpu.SemaphoreType.DMA
        h_seq, c_last = pl.pallas_call(
            functools.partial(kernel, steps, tiles, chunks, rows_n, cols_n),
            out_shape=(jax.ShapeDtypeStruct((steps, width, ch, height), jnp.bfloat16),
                       jax.ShapeDtypeStruct((width, ch, height), jnp.float32)),
            in_specs=[vmem_spec] * 4,
            out_specs=(vmem_spec, vmem_spec),
            scratch_shapes=[
                stack, stack, stack, stack,
                pltpu.VMEM((gates_n, 9 * ch), jnp.bfloat16),
                pltpu.VMEM((gates_n, height), jnp.float32),
                pltpu.VMEM((2, 2, ch, height), jnp.bfloat16),
                pltpu.VMEM((2, 16, height), jnp.bfloat16),
                pltpu.VMEM((2, len(chunks) - 1, 16, height), jnp.bfloat16),
                pltpu.VMEM((2, 8, 16, height), jnp.bfloat16),
                pltpu.VMEM((2, len(chunks) - 1, 2, 16, height), jnp.bfloat16),
                dma((2, 2)), dma((2, 2)), dma((2, 8)), dma((2, 8)),
                dma((2, len(chunks) - 1, 2)), dma((2, len(chunks) - 1, 2)),
            ],
            compiler_params=pltpu.CompilerParams(collective_id=0, has_side_effects=True, vmem_limit_bytes=32 * 1024 * 1024),
        )(h_in, c_in, w, gate_bias)
        return jnp.transpose(h_seq, (0, 3, 1, 2))[:, None], jnp.transpose(c_last, (2, 0, 1))[None]

    state_spec = P("dp", "rows", "cols", None)
    return jax.shard_map(device_fn, mesh=mesh, in_specs=(state_spec, state_spec, P(), P()), out_specs=(P(None, "dp", "rows", "cols", None), state_spec), check_vma=False)
```

```python
import functools

import jax
import jax.numpy as jnp
from jax import lax
from jax.experimental import pallas as pl
from jax.experimental.pallas import tpu as pltpu
from jax.sharding import PartitionSpec as P

UP, DOWN, LEFT, RIGHT, UP_LEFT, UP_RIGHT, DOWN_LEFT, DOWN_RIGHT = range(8)
OFFSETS = ((-1, 0), (1, 0), (0, -1), (0, 1), (-1, -1), (-1, 1), (1, -1), (1, 1))
OPPOSITE = (DOWN, UP, RIGHT, LEFT, DOWN_RIGHT, DOWN_LEFT, UP_RIGHT, UP_LEFT)
DIAGONALS = (UP_LEFT, UP_RIGHT, DOWN_LEFT, DOWN_RIGHT)
MESH = pl.DeviceIdType.MESH


def kernel(steps, tiles, rows_n, cols_n, h_init, c_init, w_ref, bias_ref, h_seq, c_last,
           hl0, hr0, hl1, hr1, ws, bs, c_strip, inner, strip, corner, ghost, recv_s, recv_d,
           send_col, recv_col, send_strip, recv_strip, send_diag, recv_diag):
    ch, lanes = h_init.shape[1], h_init.shape[2]
    cols = 2 * tiles
    groups = range(ch // 16)
    stacks = ((hl0, hr0), (hl1, hr1))
    row, col = lax.axis_index("rows"), lax.axis_index("cols")

    has, target = [], []
    for dr, dc in OFFSETS:
        r, c = row + dr, col + dc
        has.append((r >= 0) & (r < rows_n) & (c >= 0) & (c < cols_n))
        target.append({"rows": r, "cols": c})

    def at(d, action, live=None):
        pl.when(has[d] if live is None else has[d] & live)(action)

    for ref in (ghost, recv_s, recv_d):
        ref[...] = jnp.zeros_like(ref)
    barrier = pltpu.get_barrier_semaphore()
    for d in range(8):
        at(d, lambda d=d: pl.semaphore_signal(barrier, inc=1, device_id=target[d], device_id_type=MESH))
    around_r = 1 + has[UP].astype(jnp.int32) + has[DOWN].astype(jnp.int32)
    around_c = 1 + has[LEFT].astype(jnp.int32) + has[RIGHT].astype(jnp.int32)
    pl.semaphore_wait(barrier, around_r * around_c - 1)

    def column(side, j):
        return j if side == 0 else cols - 1 - j

    ws[pl.ds(0, 3 * ch), :] = w_ref[pl.ds(0, 3 * ch), :] * jnp.bfloat16(0.5)
    ws[pl.ds(3 * ch, ch), :] = w_ref[pl.ds(3 * ch, ch), :]
    scale = jnp.where(lax.broadcasted_iota(jnp.int32, (1, 4 * ch), 1) < 3 * ch, 0.5, 1.0).astype(jnp.float32)
    c_last[...] = c_init[...]

    lane = lax.broadcasted_iota(jnp.int16, (16, lanes), 1)
    lane32 = lax.broadcasted_iota(jnp.int32, (8, lanes), 1)
    even = (lane & jnp.int16(1)) == jnp.int16(0)
    ends = (lane == jnp.int16(0)) | (lane == jnp.int16(lanes - 1))

    def is_lane(n):
        return lane == jnp.int16(n)

    def roll(x, n):
        return pltpu.roll(x, n % lanes, 1) if n % lanes else x

    def part(x, g):
        return x[16 * g:16 * g + 16]

    def col_copy(p, d):
        return pltpu.make_async_remote_copy(
            src_ref=stacks[p][d - LEFT].at[1, pl.ds(ch, ch)], dst_ref=ghost.at[p, OPPOSITE[d] - LEFT],
            send_sem=send_col.at[p, d - LEFT], recv_sem=recv_col.at[p, OPPOSITE[d] - LEFT], device_id=target[d], device_id_type=MESH)

    def strip_copy(p, d):
        return pltpu.make_async_remote_copy(
            src_ref=strip.at[p], dst_ref=recv_s.at[p, OPPOSITE[d]],
            send_sem=send_strip.at[p, d], recv_sem=recv_strip.at[p, OPPOSITE[d]], device_id=target[d], device_id_type=MESH)

    def diag_copy(p, d):
        return pltpu.make_async_remote_copy(
            src_ref=corner.at[p], dst_ref=recv_d.at[p, OPPOSITE[d] - UP_LEFT],
            send_sem=send_diag.at[p, d - UP_LEFT], recv_sem=recv_diag.at[p, OPPOSITE[d] - UP_LEFT], device_id=target[d], device_id_type=MESH)

    def wait_block(ref, sem):
        pltpu.make_async_copy(ref, ref, sem).wait()

    def send_cols(p, live=None):
        for d in (LEFT, RIGHT):
            at(d, lambda d=d: col_copy(p, d).start(), live)

    def send_strip_to(p, live=None):
        for d in DIAGONALS:
            at(d, lambda d=d: diag_copy(p, d).start(), live)
        for d in (UP, DOWN):
            at(d, lambda d=d: strip_copy(p, d).start(), live)

    def wait_sends(p):
        for d in (LEFT, RIGHT):
            at(d, lambda d=d: col_copy(p, d).wait_send())
        for d in DIAGONALS:
            at(d, lambda d=d: diag_copy(p, d).wait_send())
        for d in (UP, DOWN):
            at(d, lambda d=d: strip_copy(p, d).wait_send())

    def wait_recv(p):
        for d in (UP, DOWN):
            at(d, lambda d=d: wait_block(recv_s.at[p, d], recv_strip.at[p, d]))
        for d in DIAGONALS:
            at(d, lambda d=d: wait_block(recv_d.at[p, d - UP_LEFT], recv_diag.at[p, d - UP_LEFT]))
        for d in (LEFT, RIGHT):
            at(d, lambda d=d: wait_block(ghost.at[p, d - LEFT], recv_col.at[p, d - LEFT]))

    def store_column(dst, s, g, h):
        dst[s, pl.ds(16 * g, 16)] = roll(h, 1)
        dst[s, pl.ds(ch + 16 * g, 16)] = h
        dst[s, pl.ds(2 * ch + 16 * g, 16)] = roll(h, -1)

    def add_inner(packed, x, h):
        return jnp.where(is_lane(2 * x + 3) | is_lane(2 * x + 6), roll(h, 2 * x + 5), packed)

    def store_strip(p, h):
        strip[p] = h
        block = part(h, 0)
        for g in groups[1:]:
            block = jnp.where(lax.shift_right_logical(lane & jnp.int16(63), jnp.int16(3)) == jnp.int16(g), roll(part(h, g), 8 * g), block)
        corner[p] = block

    def gates_of(stack):
        return jnp.dot(ws[...], stack, preferred_element_type=jnp.float32)

    def update(gates, c_prev):
        pre = gates + bs[...]
        in_t, forget_t, out_t, cand = (pre[ch * b:ch * b + ch] for b in range(4))
        c = (0.5 * jnp.tanh(forget_t) + 0.5) * c_prev + (0.5 * jnp.tanh(in_t) + 0.5) * jnp.tanh(cand)
        return ((0.5 * jnp.tanh(out_t) + 0.5) * jnp.tanh(c)).astype(jnp.bfloat16), c

    def strip_stack(p):
        above, here, below = [], [], []
        for g in groups:
            rows = pl.ds(16 * g, 16)
            packed, own = inner[rows], strip[p, rows]
            for side, x in ((0, -1), (1, cols)):
                h = ghost[p, side, rows]
                store_column(stacks[p][side], 0, g, h)
                packed = add_inner(packed, x, h)
                own = jnp.where(is_lane(2 * x + 6), roll(h, 2 * x + 6), own)
                own = jnp.where(is_lane(2 * x + 3), roll(h, 2 * x + 4), own)
            up = jnp.where(even, roll(recv_s[p, UP, rows], 3), packed)
            down = jnp.where(even, packed, roll(recv_s[p, DOWN, rows], -3))
            diag = [recv_d[p, k] for k in range(4)]
            up = jnp.where(is_lane(4), roll(diag[0], 4 - 65 - 8 * g), up)
            up = jnp.where(is_lane(2 * cols + 6), roll(diag[1], 2 * cols + 6 - 3 - 8 * g), up)
            down = jnp.where(is_lane(1), roll(diag[2], 1 - 68 - 8 * g), down)
            down = jnp.where(is_lane(2 * cols + 3), roll(diag[3], 2 * cols + 3 - 6 - 8 * g), down)
            above.append(up)
            here.append(own)
            below.append(down)
        rows = above + here + below
        return jnp.concatenate([roll(v, 2) for v in rows] + rows + [roll(v, -2) for v in rows], axis=0)

    def matmul(p, j):
        left, right = stacks[p]
        l_next = left[j + 2] if j + 1 < tiles else right[tiles]
        r_next = right[j + 2] if j + 1 < tiles else left[tiles]
        stack_l = jnp.concatenate([left[j], left[j + 1], l_next], axis=0)
        stack_r = jnp.concatenate([r_next, right[j + 1], right[j]], axis=0)
        return gates_of(jnp.concatenate([stack_l, stack_r], axis=1))

    def step(t, p):
        q = 1 - p
        live = t < steps - 1 if p else None
        line = bias_ref[pl.ds(t, 1), :] * scale
        bs[...] = jnp.transpose(jnp.broadcast_to(line, (lanes, line.shape[1])))
        wait_recv(p)
        hs, cs = update(gates_of(strip_stack(p)), c_strip[...])
        c_strip[...] = cs
        store_strip(q, hs)
        send_strip_to(q, live)
        merged = [jnp.where(even, part(hs, g), roll(part(hs, g), 2)) for g in groups]
        packed = [jnp.zeros((16, lanes), jnp.bfloat16) for _ in groups]
        for j in range(tiles):
            gates = matmul(p, j)
            for side in range(2):
                x = column(side, j)
                h, c = update(gates[:, side * lanes:(side + 1) * lanes], c_last[x])
                c_last[x] = c
                for g in groups:
                    fixed = jnp.where(ends, roll(merged[g], -(2 * x + 6)), part(h, g))
                    store_column(stacks[q][side], j + 1, g, fixed)
                    h_seq[t, x, pl.ds(16 * g, 16)] = fixed
                    packed[g] = add_inner(packed[g], x, fixed)
            if j == 0:
                send_cols(q, live)
        for g in groups:
            inner[pl.ds(16 * g, 16)] = packed[g]
        wait_sends(p)

    packed = [jnp.zeros((16, lanes), jnp.bfloat16) for _ in groups]
    edge = [jnp.zeros((16, lanes), jnp.bfloat16) for _ in groups]
    c_edge = [jnp.zeros((8, lanes), jnp.float32) for _ in range(ch // 8)]
    for j in range(tiles):
        for side in range(2):
            x = column(side, j)
            for g in groups:
                h = h_init[x, pl.ds(16 * g, 16)]
                store_column(stacks[0][side], j + 1, g, h)
                packed[g] = add_inner(packed[g], x, h)
                edge[g] = jnp.where(is_lane(2 * x + 5) | is_lane(2 * x + 6), roll(h, 2 * x + 6), edge[g])
            for g in range(ch // 8):
                c = roll(c_init[x, pl.ds(8 * g, 8)], 2 * x + 6)
                c_edge[g] = jnp.where((lane32 == 2 * x + 5) | (lane32 == 2 * x + 6), c, c_edge[g])
    for g in groups:
        inner[pl.ds(16 * g, 16)] = packed[g]
    for g in range(ch // 8):
        c_strip[pl.ds(8 * g, 8)] = jnp.where((lane32 & 1) == 0, c_edge[g], roll(c_edge[g], -2))
    store_strip(0, jnp.concatenate([jnp.where(even, e, roll(e, -2)) for e in edge], axis=0))
    send_strip_to(0)
    send_cols(0)

    def two_steps(i, carry):
        step(2 * i, 0)
        step(2 * i + 1, 1)
        return carry

    lax.fori_loop(0, steps // 2, two_steps, 0)
    for g in range(ch // 8):
        c = c_strip[pl.ds(8 * g, 8)]
        c = jnp.where((lane32 & 1) == 0, c, roll(c, 2))
        for x in range(cols):
            rows = pl.ds(8 * g, 8)
            c_last[x, rows] = jnp.where((lane32 == 0) | (lane32 == lanes - 1), roll(c, -(2 * x + 6)), c_last[x, rows])


def solution(mesh):
    rows_n, cols_n = mesh.shape["rows"], mesh.shape["cols"]

    def device_fn(h_init, c_init, w_rec, gate_bias):
        _, height, width, ch = h_init.shape
        steps, gates_n = gate_bias.shape
        tiles = width // 2
        w = jnp.transpose(w_rec, (3, 1, 0, 2)).reshape(gates_n, 9 * ch)
        h_in = jnp.transpose(h_init[0], (1, 2, 0))
        c_in = jnp.transpose(c_init[0], (1, 2, 0))
        stack = pltpu.VMEM((tiles + 1, 3 * ch, height), jnp.bfloat16)
        vmem_spec = pl.BlockSpec(memory_space=pltpu.VMEM)
        dma = pltpu.SemaphoreType.DMA
        h_seq, c_last = pl.pallas_call(
            functools.partial(kernel, steps, tiles, rows_n, cols_n),
            out_shape=(jax.ShapeDtypeStruct((steps, width, ch, height), jnp.bfloat16),
                       jax.ShapeDtypeStruct((width, ch, height), jnp.float32)),
            in_specs=[vmem_spec] * 4,
            out_specs=(vmem_spec, vmem_spec),
            scratch_shapes=[
                stack, stack, stack, stack,
                pltpu.VMEM((gates_n, 9 * ch), jnp.bfloat16),
                pltpu.VMEM((gates_n, height), jnp.float32),
                pltpu.VMEM((ch, height), jnp.float32),
                pltpu.VMEM((ch, height), jnp.bfloat16),
                pltpu.VMEM((2, ch, height), jnp.bfloat16),
                pltpu.VMEM((2, 16, height), jnp.bfloat16),
                pltpu.VMEM((2, 2, ch, height), jnp.bfloat16),
                pltpu.VMEM((2, 2, ch, height), jnp.bfloat16),
                pltpu.VMEM((2, 4, 16, height), jnp.bfloat16),
                dma((2, 2)), dma((2, 2)), dma((2, 2)), dma((2, 2)), dma((2, 4)), dma((2, 4)),
            ],
            compiler_params=pltpu.CompilerParams(collective_id=0, has_side_effects=True, vmem_limit_bytes=32 * 1024 * 1024),
        )(h_in, c_in, w, gate_bias)
        return jnp.transpose(h_seq, (0, 3, 1, 2))[:, None], jnp.transpose(c_last, (2, 0, 1))[None]

    state_spec = P("dp", "rows", "cols", None)
    return jax.shard_map(device_fn, mesh=mesh, in_specs=(state_spec, state_spec, P(), P()), out_specs=(P(None, "dp", "rows", "cols", None), state_spec), check_vma=False)
```

```python
import functools

import jax
import jax.numpy as jnp
from jax import lax
from jax.experimental import pallas as pl
from jax.experimental.pallas import tpu as pltpu
from jax.sharding import PartitionSpec as P

UP, DOWN, LEFT, RIGHT, UP_LEFT, UP_RIGHT, DOWN_LEFT, DOWN_RIGHT = range(8)
OFFSETS = ((-1, 0), (1, 0), (0, -1), (0, 1), (-1, -1), (-1, 1), (1, -1), (1, 1))
OPPOSITE = (DOWN, UP, RIGHT, LEFT, DOWN_RIGHT, DOWN_LEFT, UP_RIGHT, UP_LEFT)
DIAGONALS = (UP_LEFT, UP_RIGHT, DOWN_LEFT, DOWN_RIGHT)
MESH = pl.DeviceIdType.MESH


def kernel(steps, tiles, rows_n, cols_n, h_init, c_init, w_ref, bias_in, h_seq, c_last,
           hl0, hr0, hl1, hr1, ws, bias_ref, bs, c_strip, inner, strip, corner, ghost, recv_s, recv_d,
           init_sem, send_col, recv_col, send_strip, recv_strip, send_diag, recv_diag):
    ch, lanes = h_init.shape[1], h_init.shape[2]
    cols = 2 * tiles
    groups = range(ch // 16)
    stacks = ((hl0, hr0), (hl1, hr1))
    row, col = lax.axis_index("rows"), lax.axis_index("cols")

    has, target = [], []
    for dr, dc in OFFSETS:
        r, c = row + dr, col + dc
        has.append((r >= 0) & (r < rows_n) & (c >= 0) & (c < cols_n))
        target.append({"rows": r, "cols": c})

    def at(d, action, live=None):
        pl.when(has[d] if live is None else has[d] & live)(action)

    loads = [pltpu.make_async_copy(c_init, c_last, init_sem.at[0]), pltpu.make_async_copy(bias_in, bias_ref, init_sem.at[1])]
    for side in range(2):
        for j in range(tiles):
            x = j if side == 0 else cols - 1 - j
            loads.append(pltpu.make_async_copy(h_init.at[x], stacks[0][side].at[j + 1, pl.ds(ch, ch)], init_sem.at[2 + x]))
    for copy in loads:
        copy.start()

    for ref in (ghost, recv_s, recv_d):
        ref[...] = jnp.zeros_like(ref)
    barrier = pltpu.get_barrier_semaphore()
    for d in range(8):
        at(d, lambda d=d: pl.semaphore_signal(barrier, inc=1, device_id=target[d], device_id_type=MESH))
    around_r = 1 + has[UP].astype(jnp.int32) + has[DOWN].astype(jnp.int32)
    around_c = 1 + has[LEFT].astype(jnp.int32) + has[RIGHT].astype(jnp.int32)
    pl.semaphore_wait(barrier, around_r * around_c - 1)

    def column(side, j):
        return j if side == 0 else cols - 1 - j

    ws[pl.ds(0, 3 * ch), :] = w_ref[pl.ds(0, 3 * ch), :] * jnp.bfloat16(0.5)
    ws[pl.ds(3 * ch, ch), :] = w_ref[pl.ds(3 * ch, ch), :]
    scale = jnp.where(lax.broadcasted_iota(jnp.int32, (1, 4 * ch), 1) < 3 * ch, 0.5, 1.0).astype(jnp.float32)
    for copy in loads:
        copy.wait()

    lane = lax.broadcasted_iota(jnp.int16, (16, lanes), 1)
    lane32 = lax.broadcasted_iota(jnp.int32, (8, lanes), 1)
    even = (lane & jnp.int16(1)) == jnp.int16(0)
    ends = (lane == jnp.int16(0)) | (lane == jnp.int16(lanes - 1))

    def is_lane(n):
        return lane == jnp.int16(n)

    def roll(x, n):
        return pltpu.roll(x, n % lanes, 1) if n % lanes else x

    def part(x, g):
        return x[16 * g:16 * g + 16]

    def col_copy(p, d):
        return pltpu.make_async_remote_copy(
            src_ref=stacks[p][d - LEFT].at[1, pl.ds(ch, ch)], dst_ref=ghost.at[p, OPPOSITE[d] - LEFT],
            send_sem=send_col.at[p, d - LEFT], recv_sem=recv_col.at[p, OPPOSITE[d] - LEFT], device_id=target[d], device_id_type=MESH)

    def strip_copy(p, d):
        return pltpu.make_async_remote_copy(
            src_ref=strip.at[p], dst_ref=recv_s.at[p, OPPOSITE[d]],
            send_sem=send_strip.at[p, d], recv_sem=recv_strip.at[p, OPPOSITE[d]], device_id=target[d], device_id_type=MESH)

    def diag_copy(p, d):
        return pltpu.make_async_remote_copy(
            src_ref=corner.at[p], dst_ref=recv_d.at[p, OPPOSITE[d] - UP_LEFT],
            send_sem=send_diag.at[p, d - UP_LEFT], recv_sem=recv_diag.at[p, OPPOSITE[d] - UP_LEFT], device_id=target[d], device_id_type=MESH)

    def wait_block(ref, sem):
        pltpu.make_async_copy(ref, ref, sem).wait()

    def send_cols(p, live=None):
        for d in (LEFT, RIGHT):
            at(d, lambda d=d: col_copy(p, d).start(), live)

    def send_strip_to(p, live=None):
        for d in DIAGONALS:
            at(d, lambda d=d: diag_copy(p, d).start(), live)
        for d in (UP, DOWN):
            at(d, lambda d=d: strip_copy(p, d).start(), live)

    def wait_sends(p):
        for d in (LEFT, RIGHT):
            at(d, lambda d=d: col_copy(p, d).wait_send())
        for d in DIAGONALS:
            at(d, lambda d=d: diag_copy(p, d).wait_send())
        for d in (UP, DOWN):
            at(d, lambda d=d: strip_copy(p, d).wait_send())

    def wait_recv(p):
        for d in (UP, DOWN):
            at(d, lambda d=d: wait_block(recv_s.at[p, d], recv_strip.at[p, d]))
        for d in DIAGONALS:
            at(d, lambda d=d: wait_block(recv_d.at[p, d - UP_LEFT], recv_diag.at[p, d - UP_LEFT]))
        for d in (LEFT, RIGHT):
            at(d, lambda d=d: wait_block(ghost.at[p, d - LEFT], recv_col.at[p, d - LEFT]))

    def store_column(dst, s, g, h):
        dst[s, pl.ds(16 * g, 16)] = roll(h, 1)
        dst[s, pl.ds(ch + 16 * g, 16)] = h
        dst[s, pl.ds(2 * ch + 16 * g, 16)] = roll(h, -1)

    def add_inner(packed, x, h):
        return jnp.where(is_lane(2 * x + 3) | is_lane(2 * x + 6), roll(h, 2 * x + 5), packed)

    def store_strip(p, h):
        strip[p] = h
        block = part(h, 0)
        for g in groups[1:]:
            block = jnp.where(lax.shift_right_logical(lane & jnp.int16(63), jnp.int16(3)) == jnp.int16(g), roll(part(h, g), 8 * g), block)
        corner[p] = block

    def gates_of(stack):
        return jnp.dot(ws[...], stack, preferred_element_type=jnp.float32)

    def update(gates, c_prev):
        pre = gates + bs[...]
        in_t, forget_t, out_t, cand = (pre[ch * b:ch * b + ch] for b in range(4))
        c = (0.5 * jnp.tanh(forget_t) + 0.5) * c_prev + (0.5 * jnp.tanh(in_t) + 0.5) * jnp.tanh(cand)
        return ((0.5 * jnp.tanh(out_t) + 0.5) * jnp.tanh(c)).astype(jnp.bfloat16), c

    def strip_parts(p):
        own = [[roll(strip[p, pl.ds(16 * g, 16)], n) for n in (2, 0, -2)] for g in groups]
        near = [[roll(inner[pl.ds(16 * g, 16)], n) for n in (2, 0, -2)] for g in groups]
        return own, near

    def strip_stack(p, own, near):
        blocks = [[[], [], []] for _ in range(3)]
        for g in groups:
            rows = pl.ds(16 * g, 16)
            for k, n in enumerate((2, 0, -2)):
                here, packed = own[g][k], near[g][k]
                up, down = roll(recv_s[p, UP, rows], 3 + n), roll(recv_s[p, DOWN, rows], n - 3)
                if n:
                    side, x = (0, -1) if n > 0 else (1, cols)
                    top, bottom = 2 * x + 6 + n, 2 * x + 3 + n
                    h = ghost[p, side, rows]
                    here = jnp.where(is_lane(top), roll(h, top), here)
                    here = jnp.where(is_lane(bottom), roll(h, bottom + 1), here)
                    packed = jnp.where(is_lane(top) | is_lane(bottom), roll(h, top - 1), packed)
                    far = 62 if side == 0 else 0
                    up = jnp.where(is_lane(top), roll(recv_d[p, side], top - 3 - far - 8 * g), up)
                    down = jnp.where(is_lane(bottom), roll(recv_d[p, 2 + side], bottom - 6 - far - 8 * g), down)
                blocks[k][0].append(jnp.where(even, up, packed))
                blocks[k][1].append(here)
                blocks[k][2].append(jnp.where(even, packed, down))
        return jnp.concatenate([v for shift in blocks for block in shift for v in block], axis=0)

    def matmul(p, j):
        left, right = stacks[p]
        l_next = left[j + 2] if j + 1 < tiles else right[tiles]
        r_next = right[j + 2] if j + 1 < tiles else left[tiles]
        stack_l = jnp.concatenate([left[j], left[j + 1], l_next], axis=0)
        stack_r = jnp.concatenate([r_next, right[j + 1], right[j]], axis=0)
        return gates_of(jnp.concatenate([stack_l, stack_r], axis=1))

    def step(t, p):
        q = 1 - p
        live = t < steps - 1 if p else None
        line = bias_ref[pl.ds(t, 1), :] * scale
        bs[...] = jnp.transpose(jnp.broadcast_to(line, (lanes, line.shape[1])))
        own, near = strip_parts(p)
        wait_recv(p)
        for side in range(2):
            for g in groups:
                store_column(stacks[p][side], 0, g, ghost[p, side, pl.ds(16 * g, 16)])
        strip_gates = gates_of(strip_stack(p, own, near))
        hs, cs = update(strip_gates, c_strip[...])
        c_strip[...] = cs
        store_strip(q, hs)
        merged = [jnp.where(even, part(hs, g), roll(part(hs, g), 2)) for g in groups]
        packed = [jnp.zeros((16, lanes), jnp.bfloat16) for _ in groups]
        send_strip_to(q, live)
        gates = matmul(p, 0)
        for j in range(tiles):
            following = matmul(p, j + 1) if 0 < j < tiles - 1 else None
            for side in range(2):
                x = column(side, j)
                h, c = update(gates[:, side * lanes:(side + 1) * lanes], c_last[x])
                c_last[x] = c
                for g in groups:
                    fixed = jnp.where(ends, roll(merged[g], -(2 * x + 6)), part(h, g))
                    store_column(stacks[q][side], j + 1, g, fixed)
                    h_seq[t, x, pl.ds(16 * g, 16)] = fixed
                    packed[g] = add_inner(packed[g], x, fixed)
            gates = following
            if j == 0:
                send_cols(q, live)
                gates = matmul(p, 1)
        for g in groups:
            inner[pl.ds(16 * g, 16)] = packed[g]
        wait_sends(p)

    packed = [jnp.zeros((16, lanes), jnp.bfloat16) for _ in groups]
    edge = [jnp.zeros((16, lanes), jnp.bfloat16) for _ in groups]
    c_edge = [jnp.zeros((8, lanes), jnp.float32) for _ in range(ch // 8)]
    for j in range(tiles):
        for side in range(2):
            x = column(side, j)
            for g in groups:
                h = stacks[0][side][j + 1, pl.ds(ch + 16 * g, 16)]
                store_column(stacks[0][side], j + 1, g, h)
                packed[g] = add_inner(packed[g], x, h)
                edge[g] = jnp.where(is_lane(2 * x + 5) | is_lane(2 * x + 6), roll(h, 2 * x + 6), edge[g])
            for g in range(ch // 8):
                c = roll(c_last[x, pl.ds(8 * g, 8)], 2 * x + 6)
                c_edge[g] = jnp.where((lane32 == 2 * x + 5) | (lane32 == 2 * x + 6), c, c_edge[g])
    for g in groups:
        inner[pl.ds(16 * g, 16)] = packed[g]
    for g in range(ch // 8):
        c_strip[pl.ds(8 * g, 8)] = jnp.where((lane32 & 1) == 0, c_edge[g], roll(c_edge[g], -2))
    store_strip(0, jnp.concatenate([jnp.where(even, e, roll(e, -2)) for e in edge], axis=0))
    send_strip_to(0)
    send_cols(0)

    def two_steps(i, carry):
        step(2 * i, 0)
        step(2 * i + 1, 1)
        return carry

    lax.fori_loop(0, steps // 2, two_steps, 0)
    for g in range(ch // 8):
        c = c_strip[pl.ds(8 * g, 8)]
        c = jnp.where((lane32 & 1) == 0, c, roll(c, 2))
        for x in range(cols):
            rows = pl.ds(8 * g, 8)
            c_last[x, rows] = jnp.where((lane32 == 0) | (lane32 == lanes - 1), roll(c, -(2 * x + 6)), c_last[x, rows])


def solution(mesh):
    rows_n, cols_n = mesh.shape["rows"], mesh.shape["cols"]

    def device_fn(h_init, c_init, w_rec, gate_bias):
        _, height, width, ch = h_init.shape
        steps, gates_n = gate_bias.shape
        tiles = width // 2
        w = jnp.transpose(w_rec, (3, 1, 0, 2)).reshape(gates_n, 9 * ch)
        h_in = jnp.transpose(h_init[0], (1, 2, 0))
        c_in = jnp.transpose(c_init[0], (1, 2, 0))
        stack = pltpu.VMEM((tiles + 1, 3 * ch, height), jnp.bfloat16)
        hbm_spec = pl.BlockSpec(memory_space=pltpu.MemorySpace.HBM)
        vmem_spec = pl.BlockSpec(memory_space=pltpu.VMEM)
        dma = pltpu.SemaphoreType.DMA
        h_seq, c_last = pl.pallas_call(
            functools.partial(kernel, steps, tiles, rows_n, cols_n),
            out_shape=(jax.ShapeDtypeStruct((steps, width, ch, height), jnp.bfloat16),
                       jax.ShapeDtypeStruct((width, ch, height), jnp.float32)),
            in_specs=[hbm_spec, hbm_spec, vmem_spec, hbm_spec],
            out_specs=(vmem_spec, vmem_spec),
            scratch_shapes=[
                stack, stack, stack, stack,
                pltpu.VMEM((gates_n, 9 * ch), jnp.bfloat16),
                pltpu.VMEM((steps, gates_n), jnp.float32),
                pltpu.VMEM((gates_n, height), jnp.float32),
                pltpu.VMEM((ch, height), jnp.float32),
                pltpu.VMEM((ch, height), jnp.bfloat16),
                pltpu.VMEM((2, ch, height), jnp.bfloat16),
                pltpu.VMEM((2, 16, height), jnp.bfloat16),
                pltpu.VMEM((2, 2, ch, height), jnp.bfloat16),
                pltpu.VMEM((2, 2, ch, height), jnp.bfloat16),
                pltpu.VMEM((2, 4, 16, height), jnp.bfloat16),
                dma((2 + width,)), dma((2, 2)), dma((2, 2)), dma((2, 2)), dma((2, 2)), dma((2, 4)), dma((2, 4)),
            ],
            compiler_params=pltpu.CompilerParams(collective_id=0, has_side_effects=True, vmem_limit_bytes=32 * 1024 * 1024),
        )(h_in, c_in, w, gate_bias)
        return jnp.transpose(h_seq, (0, 3, 1, 2))[:, None], jnp.transpose(c_last, (2, 0, 1))[None]

    state_spec = P("dp", "rows", "cols", None)
    return jax.shard_map(device_fn, mesh=mesh, in_specs=(state_spec, state_spec, P(), P()), out_specs=(P(None, "dp", "rows", "cols", None), state_spec), check_vma=False)
```

```python
import functools

import jax
import jax.numpy as jnp
from jax import lax
from jax.experimental import pallas as pl
from jax.experimental.pallas import tpu as pltpu
from jax.sharding import PartitionSpec as P

UP, DOWN, LEFT, RIGHT, UP_LEFT, UP_RIGHT, DOWN_LEFT, DOWN_RIGHT = range(8)
OFFSETS = ((-1, 0), (1, 0), (0, -1), (0, 1), (-1, -1), (-1, 1), (1, -1), (1, 1))
OPPOSITE = (DOWN, UP, RIGHT, LEFT, DOWN_RIGHT, DOWN_LEFT, UP_RIGHT, UP_LEFT)
DIAGONALS = (UP_LEFT, UP_RIGHT, DOWN_LEFT, DOWN_RIGHT)
MESH = pl.DeviceIdType.MESH


def kernel(steps, tiles, rows_n, cols_n, h_init, c_init, w_ref, bias_ref, h_seq, c_last,
           hl0, hr0, hl1, hr1, ws, bs, c_strip, inner, strip, corner, ghost, recv_s, recv_d,
           send_col, recv_col, send_strip, recv_strip, send_diag, recv_diag):
    ch, lanes = h_init.shape[1], h_init.shape[2]
    cols = 2 * tiles
    groups = range(ch // 16)
    stacks = ((hl0, hr0), (hl1, hr1))
    row, col = lax.axis_index("rows"), lax.axis_index("cols")

    has, target = [], []
    for dr, dc in OFFSETS:
        r, c = row + dr, col + dc
        has.append((r >= 0) & (r < rows_n) & (c >= 0) & (c < cols_n))
        target.append({"rows": r, "cols": c})

    def at(d, action, live=None):
        pl.when(has[d] if live is None else has[d] & live)(action)

    for ref in (ghost, recv_s, recv_d):
        ref[...] = jnp.zeros_like(ref)
    barrier = pltpu.get_barrier_semaphore()
    for d in range(8):
        at(d, lambda d=d: pl.semaphore_signal(barrier, inc=1, device_id=target[d], device_id_type=MESH))
    around_r = 1 + has[UP].astype(jnp.int32) + has[DOWN].astype(jnp.int32)
    around_c = 1 + has[LEFT].astype(jnp.int32) + has[RIGHT].astype(jnp.int32)
    pl.semaphore_wait(barrier, around_r * around_c - 1)

    def column(side, j):
        return j if side == 0 else cols - 1 - j

    ws[pl.ds(0, 3 * ch), :] = w_ref[pl.ds(0, 3 * ch), :] * jnp.bfloat16(0.5)
    ws[pl.ds(3 * ch, ch), :] = w_ref[pl.ds(3 * ch, ch), :]
    scale = jnp.where(lax.broadcasted_iota(jnp.int32, (1, 4 * ch), 1) < 3 * ch, 0.5, 1.0).astype(jnp.float32)
    c_last[...] = c_init[...]

    lane = lax.broadcasted_iota(jnp.int16, (16, lanes), 1)
    lane32 = lax.broadcasted_iota(jnp.int32, (8, lanes), 1)
    even = (lane & jnp.int16(1)) == jnp.int16(0)
    ends = (lane == jnp.int16(0)) | (lane == jnp.int16(lanes - 1))

    def is_lane(n):
        return lane == jnp.int16(n)

    def roll(x, n):
        return pltpu.roll(x, n % lanes, 1) if n % lanes else x

    def part(x, g):
        return x[16 * g:16 * g + 16]

    def col_copy(p, d):
        return pltpu.make_async_remote_copy(
            src_ref=stacks[p][d - LEFT].at[1, pl.ds(ch, ch)], dst_ref=ghost.at[p, OPPOSITE[d] - LEFT],
            send_sem=send_col.at[p, d - LEFT], recv_sem=recv_col.at[p, OPPOSITE[d] - LEFT], device_id=target[d], device_id_type=MESH)

    def strip_copy(p, d):
        return pltpu.make_async_remote_copy(
            src_ref=strip.at[p], dst_ref=recv_s.at[p, OPPOSITE[d]],
            send_sem=send_strip.at[p, d], recv_sem=recv_strip.at[p, OPPOSITE[d]], device_id=target[d], device_id_type=MESH)

    def diag_copy(p, d):
        return pltpu.make_async_remote_copy(
            src_ref=corner.at[p], dst_ref=recv_d.at[p, OPPOSITE[d] - UP_LEFT],
            send_sem=send_diag.at[p, d - UP_LEFT], recv_sem=recv_diag.at[p, OPPOSITE[d] - UP_LEFT], device_id=target[d], device_id_type=MESH)

    def wait_block(ref, sem):
        pltpu.make_async_copy(ref, ref, sem).wait()

    def send_cols(p, live=None):
        for d in (LEFT, RIGHT):
            at(d, lambda d=d: col_copy(p, d).start(), live)

    def send_strip_to(p, live=None):
        for d in DIAGONALS:
            at(d, lambda d=d: diag_copy(p, d).start(), live)
        for d in (UP, DOWN):
            at(d, lambda d=d: strip_copy(p, d).start(), live)

    def wait_sends(p):
        for d in (LEFT, RIGHT):
            at(d, lambda d=d: col_copy(p, d).wait_send())
        for d in DIAGONALS:
            at(d, lambda d=d: diag_copy(p, d).wait_send())
        for d in (UP, DOWN):
            at(d, lambda d=d: strip_copy(p, d).wait_send())

    def wait_recv(p):
        for d in (UP, DOWN):
            at(d, lambda d=d: wait_block(recv_s.at[p, d], recv_strip.at[p, d]))
        for d in DIAGONALS:
            at(d, lambda d=d: wait_block(recv_d.at[p, d - UP_LEFT], recv_diag.at[p, d - UP_LEFT]))
        for d in (LEFT, RIGHT):
            at(d, lambda d=d: wait_block(ghost.at[p, d - LEFT], recv_col.at[p, d - LEFT]))

    def store_column(dst, s, g, h):
        dst[s, pl.ds(16 * g, 16)] = roll(h, 1)
        dst[s, pl.ds(ch + 16 * g, 16)] = h
        dst[s, pl.ds(2 * ch + 16 * g, 16)] = roll(h, -1)

    def add_inner(packed, x, h):
        return jnp.where(is_lane(2 * x + 3) | is_lane(2 * x + 6), roll(h, 2 * x + 5), packed)

    def store_strip(p, h):
        strip[p] = h
        block = part(h, 0)
        for g in groups[1:]:
            block = jnp.where(lax.shift_right_logical(lane & jnp.int16(63), jnp.int16(3)) == jnp.int16(g), roll(part(h, g), 8 * g), block)
        corner[p] = block

    def gates_of(stack):
        return jnp.dot(ws[...], stack, preferred_element_type=jnp.float32)

    def update(gates, c_prev):
        pre = gates + bs[...]
        in_t, forget_t, out_t, cand = (pre[ch * b:ch * b + ch] for b in range(4))
        c = (0.5 * jnp.tanh(forget_t) + 0.5) * c_prev + (0.5 * jnp.tanh(in_t) + 0.5) * jnp.tanh(cand)
        return ((0.5 * jnp.tanh(out_t) + 0.5) * jnp.tanh(c)).astype(jnp.bfloat16), c

    def strip_parts(p):
        own = [[roll(strip[p, pl.ds(16 * g, 16)], n) for n in (2, 0, -2)] for g in groups]
        near = [[roll(inner[pl.ds(16 * g, 16)], n) for n in (2, 0, -2)] for g in groups]
        return own, near

    def strip_stack(p, own, near):
        blocks = [[[], [], []] for _ in range(3)]
        for g in groups:
            rows = pl.ds(16 * g, 16)
            for k, n in enumerate((2, 0, -2)):
                here, packed = own[g][k], near[g][k]
                up, down = roll(recv_s[p, UP, rows], 3 + n), roll(recv_s[p, DOWN, rows], n - 3)
                if n:
                    side, x = (0, -1) if n > 0 else (1, cols)
                    top, bottom = 2 * x + 6 + n, 2 * x + 3 + n
                    h = ghost[p, side, rows]
                    here = jnp.where(is_lane(top), roll(h, top), here)
                    here = jnp.where(is_lane(bottom), roll(h, bottom + 1), here)
                    packed = jnp.where(is_lane(top) | is_lane(bottom), roll(h, top - 1), packed)
                    far = 62 if side == 0 else 0
                    up = jnp.where(is_lane(top), roll(recv_d[p, side], top - 3 - far - 8 * g), up)
                    down = jnp.where(is_lane(bottom), roll(recv_d[p, 2 + side], bottom - 6 - far - 8 * g), down)
                blocks[k][0].append(jnp.where(even, up, packed))
                blocks[k][1].append(here)
                blocks[k][2].append(jnp.where(even, packed, down))
        return jnp.concatenate([v for shift in blocks for block in shift for v in block], axis=0)

    def matmul(p, j):
        left, right = stacks[p]
        l_next = left[j + 2] if j + 1 < tiles else right[tiles]
        r_next = right[j + 2] if j + 1 < tiles else left[tiles]
        stack_l = jnp.concatenate([left[j], left[j + 1], l_next], axis=0)
        stack_r = jnp.concatenate([r_next, right[j + 1], right[j]], axis=0)
        return gates_of(jnp.concatenate([stack_l, stack_r], axis=1))

    def step(t, p):
        q = 1 - p
        live = t < steps - 1 if p else None
        line = bias_ref[pl.ds(t, 1), :] * scale
        bs[...] = jnp.transpose(jnp.broadcast_to(line, (lanes, line.shape[1])))
        own, near = strip_parts(p)
        wait_recv(p)
        for side in range(2):
            for g in groups:
                store_column(stacks[p][side], 0, g, ghost[p, side, pl.ds(16 * g, 16)])
        strip_gates = gates_of(strip_stack(p, own, near))
        hs, cs = update(strip_gates, c_strip[...])
        c_strip[...] = cs
        store_strip(q, hs)
        merged = [jnp.where(even, part(hs, g), roll(part(hs, g), 2)) for g in groups]
        packed = [jnp.zeros((16, lanes), jnp.bfloat16) for _ in groups]
        send_strip_to(q, live)
        gates = matmul(p, 0)
        for j in range(tiles):
            following = matmul(p, j + 1) if 0 < j < tiles - 1 else None
            for side in range(2):
                x = column(side, j)
                h, c = update(gates[:, side * lanes:(side + 1) * lanes], c_last[x])
                c_last[x] = c
                for g in groups:
                    fixed = jnp.where(ends, roll(merged[g], -(2 * x + 6)), part(h, g))
                    store_column(stacks[q][side], j + 1, g, fixed)
                    h_seq[t, x, pl.ds(16 * g, 16)] = fixed
                    packed[g] = add_inner(packed[g], x, fixed)
            gates = following
            if j == 0:
                send_cols(q, live)
                gates = matmul(p, 1)
        for g in groups:
            inner[pl.ds(16 * g, 16)] = packed[g]
        wait_sends(p)

    packed = [jnp.zeros((16, lanes), jnp.bfloat16) for _ in groups]
    edge = [jnp.zeros((16, lanes), jnp.bfloat16) for _ in groups]
    c_edge = [jnp.zeros((8, lanes), jnp.float32) for _ in range(ch // 8)]
    for j in range(tiles):
        for side in range(2):
            x = column(side, j)
            for g in groups:
                h = h_init[x, pl.ds(16 * g, 16)]
                store_column(stacks[0][side], j + 1, g, h)
                packed[g] = add_inner(packed[g], x, h)
                edge[g] = jnp.where(is_lane(2 * x + 5) | is_lane(2 * x + 6), roll(h, 2 * x + 6), edge[g])
            for g in range(ch // 8):
                c = roll(c_init[x, pl.ds(8 * g, 8)], 2 * x + 6)
                c_edge[g] = jnp.where((lane32 == 2 * x + 5) | (lane32 == 2 * x + 6), c, c_edge[g])
    for g in groups:
        inner[pl.ds(16 * g, 16)] = packed[g]
    for g in range(ch // 8):
        c_strip[pl.ds(8 * g, 8)] = jnp.where((lane32 & 1) == 0, c_edge[g], roll(c_edge[g], -2))
    store_strip(0, jnp.concatenate([jnp.where(even, e, roll(e, -2)) for e in edge], axis=0))
    send_strip_to(0)
    send_cols(0)

    def two_steps(i, carry):
        step(2 * i, 0)
        step(2 * i + 1, 1)
        return carry

    lax.fori_loop(0, steps // 2, two_steps, 0)
    for g in range(ch // 8):
        c = c_strip[pl.ds(8 * g, 8)]
        c = jnp.where((lane32 & 1) == 0, c, roll(c, 2))
        for x in range(cols):
            rows = pl.ds(8 * g, 8)
            c_last[x, rows] = jnp.where((lane32 == 0) | (lane32 == lanes - 1), roll(c, -(2 * x + 6)), c_last[x, rows])


def solution(mesh):
    rows_n, cols_n = mesh.shape["rows"], mesh.shape["cols"]

    def device_fn(h_init, c_init, w_rec, gate_bias):
        _, height, width, ch = h_init.shape
        steps, gates_n = gate_bias.shape
        tiles = width // 2
        w = jnp.transpose(w_rec, (3, 1, 0, 2)).reshape(gates_n, 9 * ch)
        h_in = jnp.transpose(h_init[0], (1, 2, 0))
        c_in = jnp.transpose(c_init[0], (1, 2, 0))
        stack = pltpu.VMEM((tiles + 1, 3 * ch, height), jnp.bfloat16)
        vmem_spec = pl.BlockSpec(memory_space=pltpu.VMEM)
        dma = pltpu.SemaphoreType.DMA
        h_seq, c_last = pl.pallas_call(
            functools.partial(kernel, steps, tiles, rows_n, cols_n),
            out_shape=(jax.ShapeDtypeStruct((steps, width, ch, height), jnp.bfloat16),
                       jax.ShapeDtypeStruct((width, ch, height), jnp.float32)),
            in_specs=[vmem_spec] * 4,
            out_specs=(vmem_spec, vmem_spec),
            scratch_shapes=[
                stack, stack, stack, stack,
                pltpu.VMEM((gates_n, 9 * ch), jnp.bfloat16),
                pltpu.VMEM((gates_n, height), jnp.float32),
                pltpu.VMEM((ch, height), jnp.float32),
                pltpu.VMEM((ch, height), jnp.bfloat16),
                pltpu.VMEM((2, ch, height), jnp.bfloat16),
                pltpu.VMEM((2, 16, height), jnp.bfloat16),
                pltpu.VMEM((2, 2, ch, height), jnp.bfloat16),
                pltpu.VMEM((2, 2, ch, height), jnp.bfloat16),
                pltpu.VMEM((2, 4, 16, height), jnp.bfloat16),
                dma((2, 2)), dma((2, 2)), dma((2, 2)), dma((2, 2)), dma((2, 4)), dma((2, 4)),
            ],
            compiler_params=pltpu.CompilerParams(collective_id=0, has_side_effects=True, vmem_limit_bytes=32 * 1024 * 1024),
        )(h_in, c_in, w, gate_bias)
        return jnp.transpose(h_seq, (0, 3, 1, 2))[:, None], jnp.transpose(c_last, (2, 0, 1))[None]

    state_spec = P("dp", "rows", "cols", None)
    return jax.shard_map(device_fn, mesh=mesh, in_specs=(state_spec, state_spec, P(), P()), out_specs=(P(None, "dp", "rows", "cols", None), state_spec), check_vma=False)
```

```python
import functools

import jax
import jax.numpy as jnp
from jax import lax
from jax.experimental import pallas as pl
from jax.experimental.pallas import tpu as pltpu
from jax.sharding import PartitionSpec as P

UP, DOWN, LEFT, RIGHT, UP_LEFT, UP_RIGHT, DOWN_LEFT, DOWN_RIGHT = range(8)
OFFSETS = ((-1, 0), (1, 0), (0, -1), (0, 1), (-1, -1), (-1, 1), (1, -1), (1, 1))
OPPOSITE = (DOWN, UP, RIGHT, LEFT, DOWN_RIGHT, DOWN_LEFT, UP_RIGHT, UP_LEFT)
DIAGONALS = (UP_LEFT, UP_RIGHT, DOWN_LEFT, DOWN_RIGHT)
MESH = pl.DeviceIdType.MESH


def kernel(steps, tiles, rows_n, cols_n, h_init, c_init, w_ref, bias_ref, h_seq, c_last,
           hl0, hr0, hl1, hr1, ws, bs, c_strip, inner, strip, corner, ghost, recv_s, recv_d,
           send_col, recv_col, send_strip, recv_strip, send_diag, recv_diag):
    ch, lanes = h_init.shape[1], h_init.shape[2]
    cols = 2 * tiles
    groups = range(ch // 16)
    stacks = ((hl0, hr0), (hl1, hr1))
    row, col = lax.axis_index("rows"), lax.axis_index("cols")

    has, target = [], []
    for dr, dc in OFFSETS:
        r, c = row + dr, col + dc
        has.append((r >= 0) & (r < rows_n) & (c >= 0) & (c < cols_n))
        target.append({"rows": r, "cols": c})

    def at(d, action, live=None):
        pl.when(has[d] if live is None else has[d] & live)(action)

    for ref in (ghost, recv_s, recv_d):
        ref[...] = jnp.zeros_like(ref)
    barrier = pltpu.get_barrier_semaphore()
    for d in range(8):
        at(d, lambda d=d: pl.semaphore_signal(barrier, inc=1, device_id=target[d], device_id_type=MESH))
    around_r = 1 + has[UP].astype(jnp.int32) + has[DOWN].astype(jnp.int32)
    around_c = 1 + has[LEFT].astype(jnp.int32) + has[RIGHT].astype(jnp.int32)
    pl.semaphore_wait(barrier, around_r * around_c - 1)

    def column(side, j):
        return j if side == 0 else cols - 1 - j

    ws[pl.ds(0, 3 * ch), :] = w_ref[pl.ds(0, 3 * ch), :] * jnp.bfloat16(0.5)
    ws[pl.ds(3 * ch, ch), :] = w_ref[pl.ds(3 * ch, ch), :]
    scale = jnp.where(lax.broadcasted_iota(jnp.int32, (1, 4 * ch), 1) < 3 * ch, 0.5, 1.0).astype(jnp.float32)
    c_last[...] = c_init[...]

    lane = lax.broadcasted_iota(jnp.int16, (16, lanes), 1)
    lane32 = lax.broadcasted_iota(jnp.int32, (8, lanes), 1)
    even = (lane & jnp.int16(1)) == jnp.int16(0)
    ends = (lane == jnp.int16(0)) | (lane == jnp.int16(lanes - 1))

    def is_lane(n):
        return lane == jnp.int16(n)

    def roll(x, n):
        return pltpu.roll(x, n % lanes, 1) if n % lanes else x

    def part(x, g):
        return x[16 * g:16 * g + 16]

    def col_copy(p, d):
        return pltpu.make_async_remote_copy(
            src_ref=stacks[p][d - LEFT].at[1, pl.ds(ch, ch)], dst_ref=ghost.at[p, OPPOSITE[d] - LEFT],
            send_sem=send_col.at[p, d - LEFT], recv_sem=recv_col.at[p, OPPOSITE[d] - LEFT], device_id=target[d], device_id_type=MESH)

    def strip_copy(p, d):
        return pltpu.make_async_remote_copy(
            src_ref=strip.at[p], dst_ref=recv_s.at[p, OPPOSITE[d]],
            send_sem=send_strip.at[p, d], recv_sem=recv_strip.at[p, OPPOSITE[d]], device_id=target[d], device_id_type=MESH)

    def diag_copy(p, d):
        return pltpu.make_async_remote_copy(
            src_ref=corner.at[p], dst_ref=recv_d.at[p, OPPOSITE[d] - UP_LEFT],
            send_sem=send_diag.at[p, d - UP_LEFT], recv_sem=recv_diag.at[p, OPPOSITE[d] - UP_LEFT], device_id=target[d], device_id_type=MESH)

    def wait_block(ref, sem):
        pltpu.make_async_copy(ref, ref, sem).wait()

    def send_cols(p, live=None):
        for d in (LEFT, RIGHT):
            at(d, lambda d=d: col_copy(p, d).start(), live)

    def send_strip_to(p, live=None):
        for d in DIAGONALS:
            at(d, lambda d=d: diag_copy(p, d).start(), live)

    def send_strip_rows(p, live=None):
        for d in (UP, DOWN):
            at(d, lambda d=d: strip_copy(p, d).start(), live)

    def wait_sends(p):
        for d in (LEFT, RIGHT):
            at(d, lambda d=d: col_copy(p, d).wait_send())
        for d in DIAGONALS:
            at(d, lambda d=d: diag_copy(p, d).wait_send())
        for d in (UP, DOWN):
            at(d, lambda d=d: strip_copy(p, d).wait_send())

    def wait_recv(p):
        for d in (UP, DOWN):
            at(d, lambda d=d: wait_block(recv_s.at[p, d], recv_strip.at[p, d]))
        for d in DIAGONALS:
            at(d, lambda d=d: wait_block(recv_d.at[p, d - UP_LEFT], recv_diag.at[p, d - UP_LEFT]))
        for d in (LEFT, RIGHT):
            at(d, lambda d=d: wait_block(ghost.at[p, d - LEFT], recv_col.at[p, d - LEFT]))

    def store_column(dst, s, g, h):
        dst[s, pl.ds(16 * g, 16)] = roll(h, 1)
        dst[s, pl.ds(ch + 16 * g, 16)] = h
        dst[s, pl.ds(2 * ch + 16 * g, 16)] = roll(h, -1)

    def add_inner(packed, x, h):
        return jnp.where(is_lane(2 * x + 3) | is_lane(2 * x + 6), roll(h, 2 * x + 5), packed)

    def store_strip(p, h):
        strip[p] = h
        block = part(h, 0)
        for g in groups[1:]:
            block = jnp.where(lax.shift_right_logical(lane & jnp.int16(63), jnp.int16(3)) == jnp.int16(g), roll(part(h, g), 8 * g), block)
        corner[p] = block

    def gates_of(stack):
        return jnp.dot(ws[...], stack, preferred_element_type=jnp.float32)

    def update(gates, c_prev):
        pre = gates + bs[...]
        in_t, forget_t, out_t, cand = (pre[ch * b:ch * b + ch] for b in range(4))
        c = (0.5 * jnp.tanh(forget_t) + 0.5) * c_prev + (0.5 * jnp.tanh(in_t) + 0.5) * jnp.tanh(cand)
        return ((0.5 * jnp.tanh(out_t) + 0.5) * jnp.tanh(c)).astype(jnp.bfloat16), c

    def strip_parts(p):
        own = [[roll(strip[p, pl.ds(16 * g, 16)], n) for n in (2, 0, -2)] for g in groups]
        near = [[roll(inner[pl.ds(16 * g, 16)], n) for n in (2, 0, -2)] for g in groups]
        return own, near

    def strip_stack(p, own, near):
        blocks = [[[], [], []] for _ in range(3)]
        for g in groups:
            rows = pl.ds(16 * g, 16)
            for k, n in enumerate((2, 0, -2)):
                here, packed = own[g][k], near[g][k]
                up, down = roll(recv_s[p, UP, rows], 3 + n), roll(recv_s[p, DOWN, rows], n - 3)
                if n:
                    side, x = (0, -1) if n > 0 else (1, cols)
                    top, bottom = 2 * x + 6 + n, 2 * x + 3 + n
                    h = ghost[p, side, rows]
                    here = jnp.where(is_lane(top), roll(h, top), here)
                    here = jnp.where(is_lane(bottom), roll(h, bottom + 1), here)
                    packed = jnp.where(is_lane(top) | is_lane(bottom), roll(h, top - 1), packed)
                    far = 62 if side == 0 else 0
                    up = jnp.where(is_lane(top), roll(recv_d[p, side], top - 3 - far - 8 * g), up)
                    down = jnp.where(is_lane(bottom), roll(recv_d[p, 2 + side], bottom - 6 - far - 8 * g), down)
                blocks[k][0].append(jnp.where(even, up, packed))
                blocks[k][1].append(here)
                blocks[k][2].append(jnp.where(even, packed, down))
        return jnp.concatenate([v for shift in blocks for block in shift for v in block], axis=0)

    def matmul(p, j):
        left, right = stacks[p]
        l_next = left[j + 2] if j + 1 < tiles else right[tiles]
        r_next = right[j + 2] if j + 1 < tiles else left[tiles]
        stack_l = jnp.concatenate([left[j], left[j + 1], l_next], axis=0)
        stack_r = jnp.concatenate([r_next, right[j + 1], right[j]], axis=0)
        return gates_of(jnp.concatenate([stack_l, stack_r], axis=1))

    def step(t, p):
        q = 1 - p
        live = t < steps - 1 if p else None
        line = bias_ref[pl.ds(t, 1), :] * scale
        bs[...] = jnp.transpose(jnp.broadcast_to(line, (lanes, line.shape[1])))
        own, near = strip_parts(p)
        wait_recv(p)
        for side in range(2):
            for g in groups:
                store_column(stacks[p][side], 0, g, ghost[p, side, pl.ds(16 * g, 16)])
        strip_gates = gates_of(strip_stack(p, own, near))
        hs, cs = update(strip_gates, c_strip[...])
        c_strip[...] = cs
        store_strip(q, hs)
        merged = [jnp.where(even, part(hs, g), roll(part(hs, g), 2)) for g in groups]
        packed = [jnp.zeros((16, lanes), jnp.bfloat16) for _ in groups]
        send_strip_to(q, live)
        gates = matmul(p, 0)
        for j in range(tiles):
            following = matmul(p, j + 1) if 0 < j < tiles - 1 else None
            for side in range(2):
                x = column(side, j)
                h, c = update(gates[:, side * lanes:(side + 1) * lanes], c_last[x])
                c_last[x] = c
                for g in groups:
                    fixed = jnp.where(ends, roll(merged[g], -(2 * x + 6)), part(h, g))
                    store_column(stacks[q][side], j + 1, g, fixed)
                    h_seq[t, x, pl.ds(16 * g, 16)] = fixed
                    packed[g] = add_inner(packed[g], x, fixed)
            gates = following
            if j == 0:
                send_cols(q, live)
                send_strip_rows(q, live)
                gates = matmul(p, 1)
        for g in groups:
            inner[pl.ds(16 * g, 16)] = packed[g]
        wait_sends(p)

    packed = [jnp.zeros((16, lanes), jnp.bfloat16) for _ in groups]
    edge = [jnp.zeros((16, lanes), jnp.bfloat16) for _ in groups]
    c_edge = [jnp.zeros((8, lanes), jnp.float32) for _ in range(ch // 8)]
    for j in range(tiles):
        for side in range(2):
            x = column(side, j)
            for g in groups:
                h = h_init[x, pl.ds(16 * g, 16)]
                store_column(stacks[0][side], j + 1, g, h)
                packed[g] = add_inner(packed[g], x, h)
                edge[g] = jnp.where(is_lane(2 * x + 5) | is_lane(2 * x + 6), roll(h, 2 * x + 6), edge[g])
            for g in range(ch // 8):
                c = roll(c_init[x, pl.ds(8 * g, 8)], 2 * x + 6)
                c_edge[g] = jnp.where((lane32 == 2 * x + 5) | (lane32 == 2 * x + 6), c, c_edge[g])
    for g in groups:
        inner[pl.ds(16 * g, 16)] = packed[g]
    for g in range(ch // 8):
        c_strip[pl.ds(8 * g, 8)] = jnp.where((lane32 & 1) == 0, c_edge[g], roll(c_edge[g], -2))
    store_strip(0, jnp.concatenate([jnp.where(even, e, roll(e, -2)) for e in edge], axis=0))
    send_strip_to(0)
    send_cols(0)
    send_strip_rows(0)

    def two_steps(i, carry):
        step(2 * i, 0)
        step(2 * i + 1, 1)
        return carry

    lax.fori_loop(0, steps // 2, two_steps, 0)
    for g in range(ch // 8):
        c = c_strip[pl.ds(8 * g, 8)]
        c = jnp.where((lane32 & 1) == 0, c, roll(c, 2))
        for x in range(cols):
            rows = pl.ds(8 * g, 8)
            c_last[x, rows] = jnp.where((lane32 == 0) | (lane32 == lanes - 1), roll(c, -(2 * x + 6)), c_last[x, rows])


def solution(mesh):
    rows_n, cols_n = mesh.shape["rows"], mesh.shape["cols"]

    def device_fn(h_init, c_init, w_rec, gate_bias):
        _, height, width, ch = h_init.shape
        steps, gates_n = gate_bias.shape
        tiles = width // 2
        w = jnp.transpose(w_rec, (3, 1, 0, 2)).reshape(gates_n, 9 * ch)
        h_in = jnp.transpose(h_init[0], (1, 2, 0))
        c_in = jnp.transpose(c_init[0], (1, 2, 0))
        stack = pltpu.VMEM((tiles + 1, 3 * ch, height), jnp.bfloat16)
        vmem_spec = pl.BlockSpec(memory_space=pltpu.VMEM)
        dma = pltpu.SemaphoreType.DMA
        h_seq, c_last = pl.pallas_call(
            functools.partial(kernel, steps, tiles, rows_n, cols_n),
            out_shape=(jax.ShapeDtypeStruct((steps, width, ch, height), jnp.bfloat16),
                       jax.ShapeDtypeStruct((width, ch, height), jnp.float32)),
            in_specs=[vmem_spec] * 4,
            out_specs=(vmem_spec, vmem_spec),
            scratch_shapes=[
                stack, stack, stack, stack,
                pltpu.VMEM((gates_n, 9 * ch), jnp.bfloat16),
                pltpu.VMEM((gates_n, height), jnp.float32),
                pltpu.VMEM((ch, height), jnp.float32),
                pltpu.VMEM((ch, height), jnp.bfloat16),
                pltpu.VMEM((2, ch, height), jnp.bfloat16),
                pltpu.VMEM((2, 16, height), jnp.bfloat16),
                pltpu.VMEM((2, 2, ch, height), jnp.bfloat16),
                pltpu.VMEM((2, 2, ch, height), jnp.bfloat16),
                pltpu.VMEM((2, 4, 16, height), jnp.bfloat16),
                dma((2, 2)), dma((2, 2)), dma((2, 2)), dma((2, 2)), dma((2, 4)), dma((2, 4)),
            ],
            compiler_params=pltpu.CompilerParams(collective_id=0, has_side_effects=True, vmem_limit_bytes=32 * 1024 * 1024),
        )(h_in, c_in, w, gate_bias)
        return jnp.transpose(h_seq, (0, 3, 1, 2))[:, None], jnp.transpose(c_last, (2, 0, 1))[None]

    state_spec = P("dp", "rows", "cols", None)
    return jax.shard_map(device_fn, mesh=mesh, in_specs=(state_spec, state_spec, P(), P()), out_specs=(P(None, "dp", "rows", "cols", None), state_spec), check_vma=False)
```
